128 devices in a mesh: gx: 8 (over x_lo, z), gy: 4 (over y), gz: 4 (over x_hi, core).
Axes of the slice: x: 4 (x_hi: 2, x_lo: 2; x = x_hi * 2 + x_lo), y: 4, z: 4, core: 2. Of those that a mesh axis runs over, the one named last changes fastest.
Arguments:
- inputs: bfloat16 [2560, 8192], P(('gx', 'gz'), 'gy'), may hold values from -6 to 6
- out_grad: bfloat16 [2560, 8192], P(('gx', 'gz'), 'gy'), may hold values from -6 to 6
- gate_weight: bfloat16 [8192, 16384], P('gy', ('gx', 'gz')), may hold values from -0.0625 to 0.0625
- up_weight: bfloat16 [8192, 16384], P('gy', ('gx', 'gz')), may hold values from -0.0625 to 0.0625
- down_weight: bfloat16 [16384, 8192], P(('gx', 'gz'), 'gy'), may hold values from -0.046875 to 0.046875
Outputs:
- in_grad: bfloat16 [2560, 8192], P(('gx', 'gz'), 'gy')
The draws below stay inside these ranges and needn't reach their ends.
All inputs are finite; a program needn't handle non-finite values.
Results may differ from the reference program's by a relative error of at most 0.0049.
Values may be sent and summed in bfloat16 or wider, within the bound.
A program may use at most 128 MiB of HBM per device.

```python
import jax
import jax.numpy as jnp
from jax import lax

D = 8192
FF = 16384
TOKENS = 2560


def shard_levels(rng, shape, split, least, top_value):
    gain = 1.0
    for dim, shards_of in split:
        heights = jax.random.uniform(jax.random.fold_in(jax.random.fold_in(rng, 6), dim), (shards_of,), jnp.float32, least / len(split), top_value / len(split))
        gain = gain * jnp.repeat(jnp.exp(heights), shape[dim] // shards_of).reshape((-1,) + (1,) * (len(shape) - 1 - dim))
    return gain


def bell_draw(key, shape, deviation, bound, pieces=(), held_as=jnp.bfloat16):
    factor_of = shard_levels(key, shape, pieces, -0.22, 0.18) if pieces else 1.0
    result = jax.random.normal(key, shape, jnp.float32) * deviation * factor_of
    return jnp.minimum(jnp.maximum(result, -bound), bound).astype(held_as)


def setup_inputs(seed: int = 0) -> dict:
    arg_keys = jax.random.split(jax.random.key(seed), 6)
    return {
        "inputs": bell_draw(arg_keys[0], (TOKENS, D), 1.0, 6.0, ((0, 32), (1, 4))),
        "out_grad": bell_draw(arg_keys[1], (TOKENS, D), 1.0, 6.0, ((0, 32), (1, 4))),
        "gate_weight": bell_draw(arg_keys[2], (D, FF), D ** -0.5, 0.0625, ((0, 4), (1, 32))),
        "up_weight": bell_draw(arg_keys[3], (D, FF), D ** -0.5, 0.0625, ((0, 4), (1, 32))),
        "down_weight": bell_draw(arg_keys[4], (FF, D), FF ** -0.5, 0.046875, ((0, 32), (1, 4))),
    }


def contract_last(left, right):
    return lax.dot_general(left, right, (((1,), (1,)), ((), ())), preferred_element_type=jnp.float32)


def reference(inputs, out_grad, gate_weight, up_weight, down_weight):
    gate = jnp.dot(inputs, gate_weight, preferred_element_type=jnp.float32)
    upper = jnp.dot(inputs, up_weight, preferred_element_type=jnp.float32)
    hidden_grad = contract_last(out_grad, down_weight)
    logistic = jax.nn.sigmoid(gate)
    gate_grad = (hidden_grad * upper * logistic * (1.0 + gate * (1.0 - logistic))).astype(jnp.bfloat16)
    up_grad = (hidden_grad * gate * logistic).astype(jnp.bfloat16)
    total = contract_last(gate_grad, gate_weight) + contract_last(up_grad, up_weight)
    return total.astype(jnp.bfloat16)
```

```python
import jax
import jax.numpy as jnp
from jax import lax
from jax.experimental import pallas as pl
from jax.experimental.pallas import tpu as pltpu
from jax.sharding import PartitionSpec as P

MESH = pl.DeviceIdType.MESH
F32 = jnp.float32
BF16 = jnp.bfloat16

ROWS = 80
WIDTH = 2048
HALF = WIDTH // 2
OWN = 512
Q = 256
PAIR = 2 * ROWS

GROUPS = ((0, 0), (1, 0), (1, 1), (3, 0), (3, 1), (2, 0), (2, 1), (0, 1))


def contract_last(left, right):
    return lax.dot_general(
        left, right, (((1,), (1,)), ((), ())), preferred_element_type=F32
    )


class Copies:
    def __init__(self, send_sems, recv_sems):
        self.send_sems, self.recv_sems = send_sems, recv_sems
        self.made, self.sent, self.landed = {}, [], set()

    def send(self, name, src, dst, device):
        k = len(self.made)
        copy = pltpu.make_async_remote_copy(
            src_ref=src,
            dst_ref=dst,
            send_sem=self.send_sems.at[k],
            recv_sem=self.recv_sems.at[k],
            device_id=device,
            device_id_type=MESH,
        )
        self.made[name] = copy
        self.sent.append(name)
        copy.start()

    def need(self, *names):
        for name in names:
            if name not in self.landed:
                self.landed.add(name)
                self.made[name].wait_recv()

    def free(self, *names):
        for name in names:
            if name in self.sent:
                self.sent.remove(name)
                self.made[name].wait_send()

    def finish(self):
        for name in list(self.made):
            self.need(name)
        self.free(*list(self.sent))


N_COPIES = 128
N_LOCAL = 7


def kernel(
    x_hbm, g_hbm, wg_hbm, wu_hbm, wd_hbm, out_ref,
    A, B, Wgu, Wd, S, O, ra, rb, H, sa, sb, xsa, xsb, xa, xb, zr,
    send_sems, recv_sems, local_sems,
):
    gx, y, gz = lax.axis_index("gx"), lax.axis_index("gy"), lax.axis_index("gz")
    x = lax.div(gz, 2) * 2 + lax.div(gx, 4)
    z = lax.rem(gx, 4)
    core = lax.rem(gz, 2)

    def device(dx=0, dy=0, dz=0):
        nx, ny, nz = (lax.rem(p + d + 4, 4) for p, d in ((x, dx), (y, dy), (z, dz)))
        return {
            "gx": lax.rem(nx, 2) * 4 + nz,
            "gy": ny,
            "gz": lax.div(nx, 2) * 2 + core,
        }

    partner = {"gx": gx, "gy": y, "gz": gz + 1 - 2 * core}
    xp, xm = device(dx=1), device(dx=-1)
    yp, ym = device(dy=1), device(dy=-1)
    zp, zm, zz = device(dz=1), device(dz=-1), device(dz=2)

    barrier = pltpu.get_barrier_semaphore()
    peers = (partner, xp, xm, yp, ym, zp, zm, zz)
    for peer in peers:
        pl.semaphore_signal(barrier, inc=1, device_id=peer, device_id_type=MESH)
    pl.semaphore_wait(barrier, len(peers))

    c = Copies(send_sems, recv_sems)
    L, R = pl.ds(0, HALF), pl.ds(HALF, HALF)

    c.send("Ax+", x_hbm, A.at[0, 3], xp)
    c.send("Ax-", x_hbm, A.at[0, 1], xm)
    c.send("Bz+", g_hbm, B.at[3, 0], zp)
    c.send("Bz-", g_hbm, B.at[1, 0], zm)
    locals_ = []

    def local(src, dst):
        copy = pltpu.make_async_copy(src, dst, local_sems.at[len(locals_)])
        copy.start()
        locals_.append(copy)

    local(x_hbm, A.at[0, 0])
    local(g_hbm, B.at[0, 0])
    blocks = []
    for j in range(2):
        at = pl.multiple_of((2 * core + j) * (2 * Q), 2 * Q)
        blocks.append((wg_hbm.at[:, pl.ds(j * Q, Q)], Wgu.at[:, pl.ds(at, Q)]))
        blocks.append((wu_hbm.at[:, pl.ds(j * Q, Q)], Wgu.at[:, pl.ds(at + Q, Q)]))
    blocks.append((wd_hbm, Wd.at[pl.ds(pl.multiple_of(core * OWN, OWN), OWN), :]))
    for k, (src, dst) in enumerate(blocks):
        c.send(f"w{k}", src, dst, partner)
        local(src, dst)
    c.send("Bx+0", g_hbm, B.at[0, 3], xp)
    c.send("Bx-0", g_hbm, B.at[0, 1], xm)
    c.send("Az+0", x_hbm, A.at[3, 0], zp)
    c.send("Az-0", x_hbm, A.at[1, 0], zm)

    def a_over_z(dx):
        c.send(f"Az+{dx}", A.at[0, dx], A.at[3, dx], zp)
        c.send(f"Az-{dx}", A.at[0, dx], A.at[1, dx], zm)

    def a_over_z_far(dx):
        c.need(f"Az+{dx}", f"Az-{dx}")
        c.send(f"Azf+{dx}", A.at[3, dx, :, L], A.at[2, dx, :, L], zp)
        c.send(f"Azf-{dx}", A.at[1, dx, :, R], A.at[2, dx, :, R], zm)

    def b_over_x(dz):
        c.send(f"Bx+{dz}", B.at[dz, 0], B.at[dz, 3], xp)
        c.send(f"Bx-{dz}", B.at[dz, 0], B.at[dz, 1], xm)

    def b_over_x_far(dz):
        c.need(f"Bx+{dz}", f"Bx-{dz}")
        c.send(f"Bxf+{dz}", B.at[dz, 3, :, L], B.at[dz, 2, :, L], xp)
        c.send(f"Bxf-{dz}", B.at[dz, 1, :, R], B.at[dz, 2, :, R], xm)

    def relay_0():
        c.need("Ax+", "Ax-")
        a_over_z(1)
        a_over_z(3)
        c.need("Bz+", "Bz-")
        b_over_x(1)
        c.send("Axf+", A.at[0, 3, :, L], A.at[0, 2, :, L], xp)
        c.send("Axf-", A.at[0, 1, :, R], A.at[0, 2, :, R], xm)
        c.send("Bzf+", B.at[3, 0, :, L], B.at[2, 0, :, L], zp)
        c.send("Bzf-", B.at[1, 0, :, R], B.at[2, 0, :, R], zm)

    def relay_1():
        b_over_x_far(1)
        b_over_x(3)
        c.need("Axf+", "Axf-")
        a_over_z(2)

    def relay_2():
        b_over_x_far(3)
        a_over_z_far(0)
        a_over_z_far(1)
        c.need("Bzf+", "Bzf-")
        b_over_x(2)

    def relay_3():
        a_over_z_far(3)
        a_over_z_far(2)
        b_over_x_far(0)
        b_over_x_far(2)

    relays = {0: relay_0, 1: relay_1, 2: relay_2, 3: relay_3}

    def need_tokens(dz, pair):
        if (dz, pair) == (0, 0):
            for copy in locals_:
                copy.wait()
            c.need(*(f"w{k}" for k in range(len(blocks))))
        for dx in (2 * pair, 2 * pair + 1):
            if dz == 0:
                names = {0: (), 1: ("Ax-",), 2: ("Axf+", "Axf-"), 3: ("Ax+",)}[dx]
            else:
                names = {1: (f"Az-{dx}",), 2: (f"Azf+{dx}", f"Azf-{dx}"), 3: (f"Az+{dx}",)}[dz]
            c.need(*names)
            if dx == 0:
                names = {0: (), 1: ("Bz-",), 2: ("Bzf+", "Bzf-"), 3: ("Bz+",)}[dz]
            else:
                names = {1: (f"Bx-{dz}",), 2: (f"Bxf+{dz}", f"Bxf-{dz}"), 3: (f"Bx+{dz}",)}[dx]
            c.need(*names)

    def quarter(k):
        return lax.rem(y + k, 4)

    def forward(g):
        dz, pair = GROUPS[g]
        need_tokens(dz, pair)

        @pl.loop(0, 4)
        def _(k):
            q = lax.rem(y + 2 + k, 4)
            rows_in = A[dz, 2 * pair : 2 * pair + 2].reshape(PAIR, WIDTH)
            w = Wgu[:, pl.ds(pl.multiple_of(q * 2 * Q, 2 * Q), 2 * Q)]
            S[g % 2, k, :, 0 : 2 * Q] = jnp.dot(rows_in, w, preferred_element_type=F32)
            rows_grad = B[dz, 2 * pair : 2 * pair + 2].reshape(PAIR, WIDTH)
            d = Wd[pl.ds(pl.multiple_of(q * Q, Q), Q), :]
            S[g % 2, k, :, 2 * Q : 3 * Q] = contract_last(rows_grad, d)

    def reduce_far(g):
        s = g % 2
        if g >= 2:
            c.free(f"ra+{g - 2}", f"ra-{g - 2}")
        sa[s] = S[s, 0].astype(BF16)
        c.send(f"ra+{g}", sa.at[s, pl.ds(0, ROWS)], ra.at[g, 0], yp)
        c.send(f"ra-{g}", sa.at[s, pl.ds(ROWS, ROWS)], ra.at[g, 1], ym)

    def reduce_near(g):
        s = g % 2
        if g >= 2:
            c.free(f"rb+{g - 2}", f"rb-{g - 2}")
        c.need(f"ra+{g}", f"ra-{g}")
        sb[s, 0, 0:ROWS] = (S[s, 3, 0:ROWS] + ra[g, 0].astype(F32)).astype(BF16)
        sb[s, 0, ROWS:PAIR] = S[s, 3, ROWS:PAIR].astype(BF16)
        c.send(f"rb+{g}", sb.at[s, 0], rb.at[g, 0], yp)
        sb[s, 1, 0:ROWS] = S[s, 1, 0:ROWS].astype(BF16)
        sb[s, 1, ROWS:PAIR] = (S[s, 1, ROWS:PAIR] + ra[g, 1].astype(F32)).astype(BF16)
        c.send(f"rb-{g}", sb.at[s, 1], rb.at[g, 1], ym)

    def grads(g):
        s = g % 2
        c.need(f"rb+{g}", f"rb-{g}")

        def total(at):
            cols = pl.ds(at, Q)
            return S[s, 2, :, cols] + rb[g, 0, :, cols].astype(F32) + rb[g, 1, :, cols].astype(F32)

        gate, upper, hidden_grad = total(0), total(Q), total(2 * Q)
        logistic = 1.0 / (1.0 + jnp.exp(-gate))
        scaled = hidden_grad * logistic
        at = pl.multiple_of(y * (2 * Q), 2 * Q)
        H[g, :, pl.ds(at, Q)] = (scaled * upper * (1.0 + gate * (1.0 - logistic))).astype(BF16)
        H[g, :, pl.ds(at + Q, Q)] = (scaled * gate).astype(BF16)
        own = H.at[g, :, pl.ds(at, 2 * Q)]
        c.send(f"ga+{g}", own, own, yp)
        c.send(f"ga-{g}", own, own, ym)

    def spread(g):
        c.need(f"ga+{g}", f"ga-{g}")
        at = pl.multiple_of(quarter(3) * (2 * Q), 2 * Q)
        part = H.at[g, :, pl.ds(at, Q)]
        c.send(f"gf+{g}", part, part, yp)
        at = pl.multiple_of(quarter(1) * (2 * Q), 2 * Q)
        part = H.at[g, :, pl.ds(at + Q, Q)]
        c.send(f"gf-{g}", part, part, ym)

    def backward(g):
        dz, pair = GROUPS[g]
        c.need(f"gf+{g}", f"gf-{g}")

        @pl.loop(0, 4)
        def _(n):
            at = pl.multiple_of(n * 512, 512)
            o = contract_last(H[g], Wgu[pl.ds(at, 512), :])
            O[dz, 2 * pair : 2 * pair + 2, :, pl.ds(at, 512)] = o.reshape(2, ROWS, 512)

    order = []

    def out_far(r):
        s = len(order) % 2
        order.append(r)
        if len(order) > 2:
            old = order[-3]
            c.free(f"xa+{old}", f"xa-{old}", f"xb+{old}", f"xb-{old}")
        xsa[s] = O[r, 2].astype(BF16)
        c.send(f"xa+{r}", xsa.at[s, :, L], xa.at[r, 0], xp)
        c.send(f"xa-{r}", xsa.at[s, :, R], xa.at[r, 1], xm)

    def out_near(r):
        s = order.index(r) % 2
        c.need(f"xa+{r}", f"xa-{r}")
        xsb[s, 0, :, 0:HALF] = (O[r, 1, :, 0:HALF] + xa[r, 0].astype(F32)).astype(BF16)
        xsb[s, 0, :, HALF:WIDTH] = O[r, 1, :, HALF:WIDTH].astype(BF16)
        c.send(f"xb+{r}", xsb.at[s, 0], xb.at[r, 0], xp)
        xsb[s, 1, :, 0:HALF] = O[r, 3, :, 0:HALF].astype(BF16)
        xsb[s, 1, :, HALF:WIDTH] = (O[r, 3, :, HALF:WIDTH] + xa[r, 1].astype(F32)).astype(BF16)
        c.send(f"xb-{r}", xsb.at[s, 1], xb.at[r, 1], xm)

    def out_sum(r):
        c.need(f"xb+{r}", f"xb-{r}")
        total = O[r, 0] + xb[r, 0].astype(F32) + xb[r, 1].astype(F32)
        if r == 0:
            c.need("z1", "z2", "z3")
            out_ref[...] = (total + zr[0] + zr[1] + zr[2]).astype(out_ref.dtype)
        else:
            O[r, 0] = total
            c.send(f"z{r}", O.at[r, 0], zr.at[r - 1], {1: zp, 2: zz, 3: zm}[r])

    relays[0]()
    forward(0)
    last = len(GROUPS) - 1
    finished = {g: dz for g, (dz, pair) in enumerate(GROUPS) if pair == 1}
    for t in range(last + 2):
        if t <= last:
            reduce_far(t)
        if t >= 1:
            grads(t - 1)
        if t >= 2:
            backward(t - 2)
            if t - 2 in finished:
                out_far(finished[t - 2])
        if t <= last:
            reduce_near(t)
        if t - 3 in finished:
            out_sum(finished[t - 3])
        if t + 1 <= last:
            if t + 1 in relays:
                relays[t + 1]()
            forward(t + 1)
        if t >= 1:
            spread(t - 1)
        if t - 2 in finished:
            out_near(finished[t - 2])
    backward(last)
    out_far(finished[last])
    out_sum(finished[last - 1])
    out_near(finished[last])
    out_sum(finished[last])
    c.finish()


def shards(inputs, out_grad, gate_weight, up_weight, down_weight):
    groups = len(GROUPS)
    return pl.pallas_call(
        kernel,
        out_shape=jax.ShapeDtypeStruct((ROWS, WIDTH), BF16),
        in_specs=[pl.BlockSpec(memory_space=pl.ANY)] * 5,
        out_specs=pl.BlockSpec(memory_space=pltpu.VMEM),
        scratch_shapes=[
            pltpu.VMEM((4, 4, ROWS, WIDTH), BF16),
            pltpu.VMEM((4, 4, ROWS, WIDTH), BF16),
            pltpu.VMEM((WIDTH, 8 * Q), BF16),
            pltpu.VMEM((4 * Q, WIDTH), BF16),
            pltpu.VMEM((2, 4, PAIR, 3 * Q), F32),
            pltpu.VMEM((4, 4, ROWS, WIDTH), F32),
            pltpu.VMEM((groups, 2, ROWS, 3 * Q), BF16),
            pltpu.VMEM((groups, 2, PAIR, 3 * Q), BF16),
            pltpu.VMEM((groups, PAIR, 8 * Q), BF16),
            pltpu.VMEM((2, PAIR, 3 * Q), BF16),
            pltpu.VMEM((2, 2, PAIR, 3 * Q), BF16),
            pltpu.VMEM((2, ROWS, WIDTH), BF16),
            pltpu.VMEM((2, 2, ROWS, WIDTH), BF16),
            pltpu.VMEM((4, 2, ROWS, HALF), BF16),
            pltpu.VMEM((4, 2, ROWS, WIDTH), BF16),
            pltpu.VMEM((3, ROWS, WIDTH), F32),
            pltpu.SemaphoreType.DMA((N_COPIES,)),
            pltpu.SemaphoreType.DMA((N_COPIES,)),
            pltpu.SemaphoreType.DMA((N_LOCAL,)),
        ],
        compiler_params=pltpu.CompilerParams(
            collective_id=0, has_side_effects=True, vmem_limit_bytes=66_500_000
        ),
        name="swiglu_back",
    )(inputs, out_grad, gate_weight, up_weight, down_weight)


def solution(mesh):
    return jax.shard_map(
        shards,
        mesh=mesh,
        in_specs=(
            P(("gx", "gz"), "gy"),
            P(("gx", "gz"), "gy"),
            P("gy", ("gx", "gz")),
            P("gy", ("gx", "gz")),
            P(("gx", "gz"), "gy"),
        ),
        out_specs=P(("gx", "gz"), "gy"),
        check_vma=False,
    )
```

```python
import jax
import jax.numpy as jnp
from jax import lax
from jax.experimental import pallas as pl
from jax.experimental.pallas import tpu as pltpu
from jax.sharding import PartitionSpec as P

MESH = pl.DeviceIdType.MESH
F32 = jnp.float32
BF16 = jnp.bfloat16

ROWS = 80
WIDTH = 2048
HALF = WIDTH // 2
OWN = 512
Q = 256
CUT = 3 * Q // 2

GROUPS = (
    ((0, 0, 0, 64),),
    ((1, 0, 0, 80), (3, 0, 0, 80)),
    ((1, 1, 0, 80), (1, 3, 0, 80)),
    ((3, 1, 0, 80), (3, 3, 0, 80)),
    ((1, 2, 0, 80), (3, 2, 0, 80)),
    ((2, 2, 0, 80), (2, 1, 0, 80)),
    ((2, 3, 0, 80), (2, 0, 0, 80)),
    ((0, 2, 0, 80), (0, 1, 0, 80)),
    ((0, 3, 0, 80), (0, 0, 64, 16)),
)
SIZES = tuple(sum(rows for *_, rows in group) for group in GROUPS)
STARTS = tuple(sum(SIZES[:g]) for g in range(len(SIZES)))
TOP = max(SIZES)
ALL = sum(SIZES)


def contract_last(left, right):
    return lax.dot_general(
        left, right, (((1,), (1,)), ((), ())), preferred_element_type=F32
    )


class Copies:
    def __init__(self, send_sems, recv_sems):
        self.send_sems, self.recv_sems = send_sems, recv_sems
        self.made, self.sent, self.landed = {}, [], set()

    def send(self, name, src, dst, device):
        k = len(self.made)
        copy = pltpu.make_async_remote_copy(
            src_ref=src,
            dst_ref=dst,
            send_sem=self.send_sems.at[k],
            recv_sem=self.recv_sems.at[k],
            device_id=device,
            device_id_type=MESH,
        )
        self.made[name] = copy
        self.sent.append(name)
        copy.start()

    def need(self, *names):
        for name in names:
            if name not in self.landed:
                self.landed.add(name)
                self.made[name].wait_recv()

    def free(self, *names):
        for name in names:
            if name in self.sent:
                self.sent.remove(name)
                self.made[name].wait_send()

    def finish(self):
        for name in list(self.made):
            self.need(name)
        self.free(*list(self.sent))


N_COPIES = 160
N_LOCAL = 7


def kernel(
    x_hbm, g_hbm, wg_hbm, wu_hbm, wd_hbm, out_ref,
    A, B, Wgu, Wd, S, O, ra, rb, H, sa, sb, xsa, xsb, xa, xb, zr,
    send_sems, recv_sems, local_sems,
):
    gx, y, gz = lax.axis_index("gx"), lax.axis_index("gy"), lax.axis_index("gz")
    x = lax.div(gz, 2) * 2 + lax.div(gx, 4)
    z = lax.rem(gx, 4)
    core = lax.rem(gz, 2)

    def device(dx=0, dy=0, dz=0):
        nx, ny, nz = (lax.rem(p + d + 4, 4) for p, d in ((x, dx), (y, dy), (z, dz)))
        return {
            "gx": lax.rem(nx, 2) * 4 + nz,
            "gy": ny,
            "gz": lax.div(nx, 2) * 2 + core,
        }

    partner = {"gx": gx, "gy": y, "gz": gz + 1 - 2 * core}
    xp, xm = device(dx=1), device(dx=-1)
    yp, ym = device(dy=1), device(dy=-1)
    zp, zm, zz = device(dz=1), device(dz=-1), device(dz=2)

    barrier = pltpu.get_barrier_semaphore()
    peers = (partner, xp, xm, yp, ym, zp, zm, zz)
    for peer in peers:
        pl.semaphore_signal(barrier, inc=1, device_id=peer, device_id_type=MESH)
    pl.semaphore_wait(barrier, len(peers))

    c = Copies(send_sems, recv_sems)
    L, R = pl.ds(0, HALF), pl.ds(HALF, HALF)

    c.send("Ax+", x_hbm, A.at[0, 3], xp)
    c.send("Ax-", x_hbm, A.at[0, 1], xm)
    c.send("Bz+", g_hbm, B.at[3, 0], zp)
    c.send("Bz-", g_hbm, B.at[1, 0], zm)
    c.send("Az+0", x_hbm, A.at[3, 0], zp)
    c.send("Az-0", x_hbm, A.at[1, 0], zm)
    locals_ = []

    def local(src, dst):
        copy = pltpu.make_async_copy(src, dst, local_sems.at[len(locals_)])
        copy.start()
        locals_.append(copy)

    local(x_hbm, A.at[0, 0])
    local(g_hbm, B.at[0, 0])
    blocks = []
    for j in range(2):
        at = pl.multiple_of((2 * core + j) * (2 * Q), 2 * Q)
        blocks.append((wg_hbm.at[:, pl.ds(j * Q, Q)], Wgu.at[:, pl.ds(at, Q)]))
        blocks.append((wu_hbm.at[:, pl.ds(j * Q, Q)], Wgu.at[:, pl.ds(at + Q, Q)]))
    blocks.append((wd_hbm, Wd.at[pl.ds(pl.multiple_of(core * OWN, OWN), OWN), :]))
    for k, (src, dst) in enumerate(blocks):
        c.send(f"w{k}", src, dst, partner)
        local(src, dst)

    def a_over_z(dx):
        c.send(f"Az+{dx}", A.at[0, dx], A.at[3, dx], zp)
        c.send(f"Az-{dx}", A.at[0, dx], A.at[1, dx], zm)

    def a_over_z_far(dx):
        c.need(f"Az+{dx}", f"Az-{dx}")
        c.send(f"Azf+{dx}", A.at[3, dx, :, L], A.at[2, dx, :, L], zp)
        c.send(f"Azf-{dx}", A.at[1, dx, :, R], A.at[2, dx, :, R], zm)

    def b_over_x(dz):
        c.send(f"Bx+{dz}", B.at[dz, 0], B.at[dz, 3], xp)
        c.send(f"Bx-{dz}", B.at[dz, 0], B.at[dz, 1], xm)

    def b_over_x_far(dz):
        c.need(f"Bx+{dz}", f"Bx-{dz}")
        c.send(f"Bxf+{dz}", B.at[dz, 3, :, L], B.at[dz, 2, :, L], xp)
        c.send(f"Bxf-{dz}", B.at[dz, 1, :, R], B.at[dz, 2, :, R], xm)

    def relay_0():
        c.need("Ax+", "Ax-")
        c.send("Axf+", A.at[0, 3, :, L], A.at[0, 2, :, L], xp)
        c.send("Axf-", A.at[0, 1, :, R], A.at[0, 2, :, R], xm)
        a_over_z(1)
        a_over_z(3)
        c.need("Bz+", "Bz-")
        b_over_x(1)
        b_over_x(3)
        c.send("Bzf+", B.at[3, 0, :, L], B.at[2, 0, :, L], zp)
        c.send("Bzf-", B.at[1, 0, :, R], B.at[2, 0, :, R], zm)

    def relay_2():
        c.need("Axf+", "Axf-")
        a_over_z(2)
        b_over_x_far(1)
        b_over_x_far(3)

    def relay_3():
        a_over_z_far(0)
        a_over_z_far(1)
        a_over_z_far(3)
        c.need("Bzf+", "Bzf-")
        b_over_x(2)

    def relay_4():
        a_over_z_far(2)
        b_over_x_far(2)
        b_over_x(0)

    def relay_5():
        b_over_x_far(0)

    relays = {0: relay_0, 2: relay_2, 3: relay_3, 4: relay_4, 5: relay_5}

    def need_tokens(g):
        if g == 0:
            for copy in locals_:
                copy.wait()
            c.need(*(f"w{k}" for k in range(len(blocks))))
        for dz, dx, *_ in GROUPS[g]:
            if dz == 0:
                c.need(*{0: (), 1: ("Ax-",), 2: ("Axf+", "Axf-"), 3: ("Ax+",)}[dx])
            else:
                c.need(*{1: (f"Az-{dx}",), 2: (f"Azf+{dx}", f"Azf-{dx}"), 3: (f"Az+{dx}",)}[dz])
            if dx == 0:
                c.need(*{0: (), 1: ("Bz-",), 2: ("Bzf+", "Bzf-"), 3: ("Bz+",)}[dz])
            else:
                c.need(*{1: (f"Bx-{dz}",), 2: (f"Bxf+{dz}", f"Bxf-{dz}"), 3: (f"Bx+{dz}",)}[dx])

    def rows_of(ref, g):
        parts = [ref[dz, dx, first : first + rows] for dz, dx, first, rows in GROUPS[g]]
        return parts[0] if len(parts) == 1 else jnp.concatenate(parts, axis=0)

    def quarter(k):
        return lax.rem(y + k, 4)

    def forward(g):
        m = SIZES[g]
        need_tokens(g)

        @pl.loop(0, 4)
        def _(k):
            q = lax.rem(y + 2 + k, 4)
            w = Wgu[:, pl.ds(pl.multiple_of(q * 2 * Q, 2 * Q), 2 * Q)]
            S[g % 2, k, 0:m, 0 : 2 * Q] = jnp.dot(rows_of(A, g), w, preferred_element_type=F32)
            d = Wd[pl.ds(pl.multiple_of(q * Q, Q), Q), :]
            S[g % 2, k, 0:m, 2 * Q : 3 * Q] = contract_last(rows_of(B, g), d)

    def reduce_far(g):
        s, m = g % 2, SIZES[g]
        at = pl.ds(STARTS[g], m)
        if g >= 2:
            c.free(f"ra+{g - 2}", f"ra-{g - 2}")
        sa[s, 0:m] = S[s, 0, 0:m].astype(BF16)
        c.send(f"ra+{g}", sa.at[s, pl.ds(0, m), pl.ds(0, CUT)], ra.at[0, at], yp)
        c.send(f"ra-{g}", sa.at[s, pl.ds(0, m), pl.ds(CUT, CUT)], ra.at[1, at], ym)

    def reduce_near(g):
        s, m = g % 2, SIZES[g]
        at = slice(STARTS[g], STARTS[g] + m)
        if g >= 2:
            c.free(f"rb+{g - 2}", f"rb-{g - 2}")
        c.need(f"ra+{g}", f"ra-{g}")
        sb[s, 0, 0:m, 0:CUT] = (S[s, 3, 0:m, 0:CUT] + ra[0, at].astype(F32)).astype(BF16)
        sb[s, 0, 0:m, CUT:] = S[s, 3, 0:m, CUT:].astype(BF16)
        c.send(f"rb+{g}", sb.at[s, 0, pl.ds(0, m)], rb.at[0, pl.ds(STARTS[g], m)], yp)
        sb[s, 1, 0:m, 0:CUT] = S[s, 1, 0:m, 0:CUT].astype(BF16)
        sb[s, 1, 0:m, CUT:] = (S[s, 1, 0:m, CUT:] + ra[1, at].astype(F32)).astype(BF16)
        c.send(f"rb-{g}", sb.at[s, 1, pl.ds(0, m)], rb.at[1, pl.ds(STARTS[g], m)], ym)

    def grads(g):
        s, m = g % 2, SIZES[g]
        rows = pl.ds(STARTS[g], m)
        c.need(f"rb+{g}", f"rb-{g}")

        def total(at):
            cols = pl.ds(at, Q)
            return S[s, 2, 0:m, cols] + rb[0, rows, cols].astype(F32) + rb[1, rows, cols].astype(F32)

        gate, upper, hidden_grad = total(0), total(Q), total(2 * Q)
        logistic = 1.0 / (1.0 + jnp.exp(-gate))
        scaled = hidden_grad * logistic
        at = pl.multiple_of(y * (2 * Q), 2 * Q)
        H[rows, pl.ds(at, Q)] = (scaled * upper * (1.0 + gate * (1.0 - logistic))).astype(BF16)
        H[rows, pl.ds(at + Q, Q)] = (scaled * gate).astype(BF16)
        own = H.at[rows, pl.ds(at, 2 * Q)]
        c.send(f"ga+{g}", own, own, yp)
        c.send(f"ga-{g}", own, own, ym)

    def spread(g):
        rows = pl.ds(STARTS[g], SIZES[g])
        c.need(f"ga+{g}", f"ga-{g}")
        at = pl.multiple_of(quarter(3) * (2 * Q), 2 * Q)
        part = H.at[rows, pl.ds(at, Q)]
        c.send(f"gf+{g}", part, part, yp)
        at = pl.multiple_of(quarter(1) * (2 * Q), 2 * Q)
        part = H.at[rows, pl.ds(at + Q, Q)]
        c.send(f"gf-{g}", part, part, ym)

    def backward(g):
        c.need(f"gf+{g}", f"gf-{g}")

        @pl.loop(0, 4)
        def _(n):
            cols = pl.ds(pl.multiple_of(n * 512, 512), 512)
            o = contract_last(H[STARTS[g] : STARTS[g] + SIZES[g]], Wgu[cols, :])
            done = 0
            for dz, dx, first, rows in GROUPS[g]:
                O[dz, dx, first : first + rows, cols] = o[done : done + rows]
                done += rows

    def out_far(r):
        xsa[r] = O[r, 2].astype(BF16)
        c.send(f"xa+{r}", xsa.at[r, :, L], xa.at[r, 0], xp)
        c.send(f"xa-{r}", xsa.at[r, :, R], xa.at[r, 1], xm)

    def out_plus(r):
        c.need(f"xa+{r}")
        xsb[r, 0, :, 0:HALF] = (O[r, 1, :, 0:HALF] + xa[r, 0].astype(F32)).astype(BF16)
        xsb[r, 0, :, HALF:WIDTH] = O[r, 1, :, HALF:WIDTH].astype(BF16)
        c.send(f"xb+{r}", xsb.at[r, 0], xb.at[r, 0], xp)

    def out_minus(r):
        c.need(f"xa-{r}")
        xsb[r, 1, :, 0:HALF] = O[r, 3, :, 0:HALF].astype(BF16)
        xsb[r, 1, :, HALF:WIDTH] = (O[r, 3, :, HALF:WIDTH] + xa[r, 1].astype(F32)).astype(BF16)
        c.send(f"xb-{r}", xsb.at[r, 1], xb.at[r, 1], xm)

    def out_sum(r):
        c.need(f"xb+{r}", f"xb-{r}")
        total = O[r, 0] + xb[r, 0].astype(F32) + xb[r, 1].astype(F32)
        if r == 0:
            c.need("z1", "z2", "z3")
            out_ref[...] = (total + zr[0] + zr[1] + zr[2]).astype(out_ref.dtype)
        else:
            O[r, 0] = total
            c.send(f"z{r}", O.at[r, 0], zr.at[r - 1], {1: zp, 2: zz, 3: zm}[r])

    after = {4: ((out_far, 1), (out_far, 3)), 5: ((out_far, 2),), 7: ((out_far, 0),)}
    later = {
        4: ((out_plus, 1), (out_minus, 1), (out_plus, 3), (out_minus, 3)),
        5: ((out_sum, 1), (out_sum, 3), (out_plus, 2)),
        6: ((out_minus, 2),),
    }

    def run(events):
        for event, r in events:
            event(r)

    relays[0]()
    forward(0)
    last = len(GROUPS) - 1
    for t in range(last + 2):
        if t <= last:
            reduce_far(t)
        if t >= 1:
            grads(t - 1)
        if t >= 2:
            backward(t - 2)
            run(after.get(t - 2, ()))
        if t <= last:
            reduce_near(t)
        if t + 1 <= last:
            if t + 1 in relays:
                relays[t + 1]()
            forward(t + 1)
        if t >= 1:
            spread(t - 1)
        run(later.get(t - 2, ()))
    out_sum(2)
    backward(last)
    out_minus(0)
    out_plus(0)
    out_sum(0)
    c.finish()


def shards(inputs, out_grad, gate_weight, up_weight, down_weight):
    return pl.pallas_call(
        kernel,
        out_shape=jax.ShapeDtypeStruct((ROWS, WIDTH), BF16),
        in_specs=[pl.BlockSpec(memory_space=pl.ANY)] * 5,
        out_specs=pl.BlockSpec(memory_space=pltpu.VMEM),
        scratch_shapes=[
            pltpu.VMEM((4, 4, ROWS, WIDTH), BF16),
            pltpu.VMEM((4, 4, ROWS, WIDTH), BF16),
            pltpu.VMEM((WIDTH, 8 * Q), BF16),
            pltpu.VMEM((4 * Q, WIDTH), BF16),
            pltpu.VMEM((2, 4, TOP, 3 * Q), F32),
            pltpu.VMEM((4, 4, ROWS, WIDTH), F32),
            pltpu.VMEM((2, ALL, CUT), BF16),
            pltpu.VMEM((2, ALL, 3 * Q), BF16),
            pltpu.VMEM((ALL, 8 * Q), BF16),
            pltpu.VMEM((2, TOP, 3 * Q), BF16),
            pltpu.VMEM((2, 2, TOP, 3 * Q), BF16),
            pltpu.VMEM((4, ROWS, WIDTH), BF16),
            pltpu.VMEM((4, 2, ROWS, WIDTH), BF16),
            pltpu.VMEM((4, 2, ROWS, HALF), BF16),
            pltpu.VMEM((4, 2, ROWS, WIDTH), BF16),
            pltpu.VMEM((3, ROWS, WIDTH), F32),
            pltpu.SemaphoreType.DMA((N_COPIES,)),
            pltpu.SemaphoreType.DMA((N_COPIES,)),
            pltpu.SemaphoreType.DMA((N_LOCAL,)),
        ],
        compiler_params=pltpu.CompilerParams(
            collective_id=0, has_side_effects=True, vmem_limit_bytes=66_500_000
        ),
        name="swiglu_back",
    )(inputs, out_grad, gate_weight, up_weight, down_weight)


def solution(mesh):
    return jax.shard_map(
        shards,
        mesh=mesh,
        in_specs=(
            P(("gx", "gz"), "gy"),
            P(("gx", "gz"), "gy"),
            P("gy", ("gx", "gz")),
            P("gy", ("gx", "gz")),
            P(("gx", "gz"), "gy"),
        ),
        out_specs=P(("gx", "gz"), "gy"),
        check_vma=False,
    )
```

```python
import jax
import jax.numpy as jnp
from jax import lax
from jax.experimental import pallas as pl
from jax.experimental.pallas import tpu as pltpu
from jax.sharding import PartitionSpec as P

MESH = pl.DeviceIdType.MESH
F32 = jnp.float32
BF16 = jnp.bfloat16

ROWS = 80
WIDTH = 2048
HALF = WIDTH // 2
OWN = 512
Q = 256
CUT = 3 * Q // 2

GROUPS = (
    ((0, 0, 0, 80),),
    ((0, 1, 0, 48), (0, 3, 0, 48)),
    ((1, 0, 0, 48), (3, 0, 0, 48)),
    ((1, 1, 0, 80), (3, 3, 0, 80)),
    ((1, 3, 0, 80), (3, 1, 0, 80)),
    ((2, 2, 0, 80), (1, 2, 0, 80), (2, 1, 0, 48)),
    ((3, 2, 0, 80), (2, 3, 0, 80), (2, 1, 48, 32)),
    ((0, 2, 0, 80), (2, 0, 0, 80)),
    ((1, 0, 48, 32), (3, 0, 48, 32), (0, 1, 48, 32), (0, 3, 48, 32)),
)
EARLY = 48
SIZES = tuple(sum(rows for *_, rows in group) for group in GROUPS)
STARTS = tuple(sum(SIZES[:g]) for g in range(len(SIZES)))
TOP = max(SIZES)
ALL = sum(SIZES)


def contract_last(left, right):
    return lax.dot_general(
        left, right, (((1,), (1,)), ((), ())), preferred_element_type=F32
    )


class Copies:
    def __init__(self, send_sems, recv_sems):
        self.send_sems, self.recv_sems = send_sems, recv_sems
        self.made, self.sent, self.landed = {}, {}, set()
        self.keys, self.user = {}, {}

    def send(self, name, src, dst, device):
        k = len(self.made) % SENDS
        for old in [old for old, at in self.sent.items() if at == k]:
            self.free(old)
        key = name[:3] + str(int(name[3:]) % 3) if name[:2] in OVER_Y else name
        r = self.keys.setdefault(key, len(self.keys))
        assert self.user.get(key, name) == name or self.user[key] in self.landed
        self.user[key] = name
        copy = pltpu.make_async_remote_copy(
            src_ref=src,
            dst_ref=dst,
            send_sem=self.send_sems.at[k],
            recv_sem=self.recv_sems.at[r],
            device_id=device,
            device_id_type=MESH,
        )
        self.made[name] = copy
        self.sent[name] = k
        copy.start()

    def need(self, *names):
        for name in names:
            if name not in self.landed:
                self.landed.add(name)
                self.made[name].wait_recv()

    def free(self, *names):
        for name in names:
            if name in self.sent:
                del self.sent[name]
                self.made[name].wait_send()

    def finish(self):
        assert len(self.keys) == RECVS
        self.need(*self.made)
        self.free(*list(self.sent))


OVER_Y = ("ra", "rb", "ga", "gf")
SENDS = 40
RECVS = 104


def kernel(
    x_hbm, g_hbm, wg_hbm, wu_hbm, wd_hbm, out_ref,
    A, B, Wgu, Wd, S, O, ra, rb, H, sa, sb, xsa, xsb, xa, xb, xd, zs, zt, zr,
    send_sems, recv_sems, local_sems, weight_sends, weight_sems,
):
    gx, y, gz = lax.axis_index("gx"), lax.axis_index("gy"), lax.axis_index("gz")
    x = lax.div(gz, 2) * 2 + lax.div(gx, 4)
    z = lax.rem(gx, 4)
    core = lax.rem(gz, 2)

    def device(dx=0, dy=0, dz=0):
        nx, ny, nz = (lax.rem(p + d + 4, 4) for p, d in ((x, dx), (y, dy), (z, dz)))
        return {
            "gx": lax.rem(nx, 2) * 4 + nz,
            "gy": ny,
            "gz": lax.div(nx, 2) * 2 + core,
        }

    partner = {"gx": gx, "gy": y, "gz": gz + 1 - 2 * core}
    xp, xm = device(dx=1), device(dx=-1)
    yp, ym = device(dy=1), device(dy=-1)
    zp, zm = device(dz=1), device(dz=-1)

    barrier = pltpu.get_barrier_semaphore()
    peers = (partner, xp, xm, yp, ym, zp, zm)
    own_tokens = [
        pltpu.make_async_copy(src, ref.at[0, 0], local_sems.at[k])
        for k, (src, ref) in enumerate(((x_hbm, A), (g_hbm, B)))
    ]
    for copy in own_tokens:
        copy.start()
    for peer in peers:
        pl.semaphore_signal(barrier, inc=1, device_id=peer, device_id_type=MESH)
    pl.semaphore_wait(barrier, len(peers))

    c = Copies(send_sems, recv_sems)
    L, R = pl.ds(0, HALF), pl.ds(HALF, HALF)

    near = lax.rem(y + 2, 4)
    mine = 1 - jnp.abs(lax.div(near, 2) - core)
    lead = mine * lax.rem(near, 2)
    locals_ = []

    def local(src, dst, sem):
        copy = pltpu.make_async_copy(src, dst, sem)
        copy.start()
        return copy

    def pieces(q, j):
        wide, narrow = pl.multiple_of(q * 2 * Q, 2 * Q), pl.multiple_of(q * Q, Q)
        part = pl.ds(pl.multiple_of(j * Q, Q), Q)
        return (
            (wg_hbm.at[:, part], Wgu.at[:, pl.ds(wide, Q)]),
            (wu_hbm.at[:, part], Wgu.at[:, pl.ds(wide + Q, Q)]),
            (wd_hbm.at[part], Wd.at[pl.ds(narrow, Q)]),
        )

    own = [(2 * core + j, j) for j in (lead, 1 - lead)]
    for n, (q, j) in enumerate(own):
        for k, (src, dst) in enumerate(pieces(q, j)):
            copy = pltpu.make_async_remote_copy(
                src_ref=src,
                dst_ref=dst,
                send_sem=weight_sends.at[3 * n + k],
                recv_sem=weight_sems.at[3 * q + k],
                device_id=partner,
                device_id_type=MESH,
            )
            copy.start()
            locals_.append(copy)

    def own_over_x(name, hbm, ref, rows):
        c.send(name.replace("@", "+"), hbm.at[rows], ref.at[0, 3, rows], xp)
        c.send(name.replace("@", "-"), hbm.at[rows], ref.at[0, 1, rows], xm)

    def own_over_z(name, hbm, ref, rows):
        c.send(name.replace("@", "+"), hbm.at[rows], ref.at[3, 0, rows], zp)
        c.send(name.replace("@", "-"), hbm.at[rows], ref.at[1, 0, rows], zm)

    ahead, behind = pl.ds(0, EARLY), pl.ds(EARLY, ROWS - EARLY)
    own_over_x("Ax@", x_hbm, A, ahead)
    own_over_z("Bz@", g_hbm, B, ahead)
    own_over_x("Bx@0", g_hbm, B, ahead)
    own_over_z("Az@0", x_hbm, A, ahead)
    own_over_x("Ax@b", x_hbm, A, behind)
    own_over_z("Bz@b", g_hbm, B, behind)

    def need_weights(q):
        for k, (src, dst) in enumerate(pieces(q, 0)):
            pltpu.make_async_copy(src, dst, weight_sems.at[3 * q + k]).wait()

    def a_over_z(dx):
        c.send(f"Az+{dx}", A.at[0, dx], A.at[3, dx], zp)
        c.send(f"Az-{dx}", A.at[0, dx], A.at[1, dx], zm)

    def a_over_z_far(dx):
        c.need(f"Az+{dx}", f"Az-{dx}")
        if dx == 0:
            c.need("Az+0b", "Az-0b")
        c.send(f"Azf+{dx}", A.at[3, dx, :, L], A.at[2, dx, :, L], zp)
        c.send(f"Azf-{dx}", A.at[1, dx, :, R], A.at[2, dx, :, R], zm)

    def b_over_x(dz):
        c.send(f"Bx+{dz}", B.at[dz, 0], B.at[dz, 3], xp)
        c.send(f"Bx-{dz}", B.at[dz, 0], B.at[dz, 1], xm)

    def b_over_x_far(dz):
        c.need(f"Bx+{dz}", f"Bx-{dz}")
        if dz == 0:
            c.need("Bx+0b", "Bx-0b")
        c.send(f"Bxf+{dz}", B.at[dz, 3, :, L], B.at[dz, 2, :, L], xp)
        c.send(f"Bxf-{dz}", B.at[dz, 1, :, R], B.at[dz, 2, :, R], xm)

    def relay_1():
        c.need("Ax+", "Ax-", "Ax+b", "Ax-b")
        c.send("Az-1", A.at[0, 1], A.at[1, 1], zm)
        c.send("Az+3", A.at[0, 3], A.at[3, 3], zp)
        c.need("Bz+", "Bz-", "Bz+b", "Bz-b")
        c.send("Bx-1", B.at[1, 0], B.at[1, 1], xm)
        c.send("Bx+3", B.at[3, 0], B.at[3, 3], xp)
        c.send("Axf+", A.at[0, 3, :, L], A.at[0, 2, :, L], xp)
        c.send("Axf-", A.at[0, 1, :, R], A.at[0, 2, :, R], xm)
        c.send("Bzf+", B.at[3, 0, :, L], B.at[2, 0, :, L], zp)
        c.send("Bzf-", B.at[1, 0, :, R], B.at[2, 0, :, R], zm)
        c.send("Az+1", A.at[0, 1], A.at[3, 1], zp)
        c.send("Az-3", A.at[0, 3], A.at[1, 3], zm)
        c.send("Bx+1", B.at[1, 0], B.at[1, 3], xp)
        c.send("Bx-3", B.at[3, 0], B.at[3, 1], xm)

    def relay_2():
        c.need("Bzf+", "Bzf-")
        b_over_x(2)
        c.need("Axf+", "Axf-")
        a_over_z(2)

    def relay_3():
        b_over_x_far(1)
        a_over_z_far(1)

    def relay_4():
        a_over_z_far(2)
        b_over_x_far(2)
        a_over_z_far(3)
        b_over_x_far(3)
        own_over_z("Az@0b", x_hbm, A, behind)

    def relay_5():
        own_over_x("Bx@0b", g_hbm, B, behind)

    def relay_6():
        a_over_z_far(0)
        b_over_x_far(0)

    relays = {5: relay_5, 6: relay_6}

    def need_tokens(g):
        for dz, dx, first, _ in GROUPS[g]:
            late = first >= EARLY
            if dz == 0:
                c.need(*{0: (), 1: ("Ax-", "Bx-0"), 2: ("Axf+", "Axf-", "Bxf+0", "Bxf-0"), 3: ("Ax+", "Bx+0")}[dx])
                if late:
                    c.need(*{0: (), 1: ("Ax-b", "Bx-0b"), 2: (), 3: ("Ax+b", "Bx+0b")}[dx])
                continue
            c.need(*{1: (f"Az-{dx}",), 2: (f"Azf+{dx}", f"Azf-{dx}"), 3: (f"Az+{dx}",)}[dz])
            if dx == 0:
                c.need(*{1: ("Bz-",), 2: ("Bzf+", "Bzf-"), 3: ("Bz+",)}[dz])
                if late:
                    c.need(*{1: ("Az-0b", "Bz-b"), 2: (), 3: ("Az+0b", "Bz+b")}[dz])
            else:
                c.need(*{1: (f"Bx-{dz}",), 2: (f"Bxf+{dz}", f"Bxf-{dz}"), 3: (f"Bx+{dz}",)}[dx])

    def rows_of(ref, g):
        parts = [ref[dz, dx, first : first + rows] for dz, dx, first, rows in GROUPS[g]]
        return parts[0] if len(parts) == 1 else jnp.concatenate(parts, axis=0)

    def quarter(k):
        return lax.rem(y + k, 4)

    def forward(g, start=0, stop=4):
        m = SIZES[g]
        need_tokens(g)

        @pl.loop(start, stop)
        def _(k):
            q = lax.rem(y + 2 + k, 4)
            if g == 0:
                need_weights(q)
            w = Wgu[:, pl.ds(pl.multiple_of(q * 2 * Q, 2 * Q), 2 * Q)]
            S[g % 2, k, 0:m, 0 : 2 * Q] = jnp.dot(rows_of(A, g), w, preferred_element_type=F32)
            d = Wd[pl.ds(pl.multiple_of(q * Q, Q), Q), :]
            S[g % 2, k, 0:m, 2 * Q : 3 * Q] = contract_last(rows_of(B, g), d)

    def reduce_far(g):
        s, m = g % 2, SIZES[g]
        at = pl.ds(STARTS[g], m)
        if g >= 2:
            c.free(f"ra+{g - 2}", f"ra-{g - 2}")
        sa[s, 0:m] = S[s, 0, 0:m].astype(BF16)
        c.send(f"ra+{g}", sa.at[s, pl.ds(0, m), pl.ds(0, CUT)], ra.at[0, at], yp)
        c.send(f"ra-{g}", sa.at[s, pl.ds(0, m), pl.ds(CUT, CUT)], ra.at[1, at], ym)

    def reduce_near(g):
        s, m = g % 2, SIZES[g]
        at = slice(STARTS[g], STARTS[g] + m)
        if g >= 2:
            c.free(f"rb+{g - 2}", f"rb-{g - 2}")
        c.need(f"ra+{g}", f"ra-{g}")
        sb[s, 0, 0:m, 0:CUT] = (S[s, 3, 0:m, 0:CUT] + ra[0, at].astype(F32)).astype(BF16)
        sb[s, 0, 0:m, CUT:] = S[s, 3, 0:m, CUT:].astype(BF16)
        c.send(f"rb+{g}", sb.at[s, 0, pl.ds(0, m)], rb.at[0, pl.ds(STARTS[g], m)], yp)
        sb[s, 1, 0:m, 0:CUT] = S[s, 1, 0:m, 0:CUT].astype(BF16)
        sb[s, 1, 0:m, CUT:] = (S[s, 1, 0:m, CUT:] + ra[1, at].astype(F32)).astype(BF16)
        c.send(f"rb-{g}", sb.at[s, 1, pl.ds(0, m)], rb.at[1, pl.ds(STARTS[g], m)], ym)

    last = len(GROUPS) - 1

    def grads(g):
        s, m = g % 2, SIZES[g]
        rows = pl.ds(STARTS[g], m)
        c.need(f"rb+{g}", f"rb-{g}")

        def total(at):
            cols = pl.ds(at, Q)
            return S[s, 2, 0:m, cols] + rb[0, rows, cols].astype(F32) + rb[1, rows, cols].astype(F32)

        gate, upper, hidden_grad = total(0), total(Q), total(2 * Q)
        logistic = 1.0 / (1.0 + jnp.exp(-gate))
        scaled = hidden_grad * logistic
        at = pl.multiple_of(y * (2 * Q), 2 * Q)
        H[rows, pl.ds(at, Q)] = (scaled * upper * (1.0 + gate * (1.0 - logistic))).astype(BF16)
        H[rows, pl.ds(at + Q, Q)] = (scaled * gate).astype(BF16)
        own = H.at[rows, pl.ds(at, 2 * Q)]
        c.send(f"ga+{g}", own, own, yp)
        c.send(f"ga-{g}", own, own, ym)

    def spread(g):
        rows = pl.ds(STARTS[g], SIZES[g])
        c.need(f"ga+{g}", f"ga-{g}")
        at = pl.multiple_of(quarter(3) * (2 * Q), 2 * Q)
        part = H.at[rows, pl.ds(at, Q)]
        c.send(f"gf+{g}", part, part, yp)
        at = pl.multiple_of(quarter(1) * (2 * Q), 2 * Q)
        part = H.at[rows, pl.ds(at + Q, Q)]
        c.send(f"gf-{g}", part, part, ym)

    def product(g, start=0, steps=4):
        rows = slice(STARTS[g], STARTS[g] + SIZES[g])
        c.need(f"gf+{g}", f"gf-{g}")

        @pl.loop(start, start + steps)
        def _(n):
            cols = pl.ds(pl.multiple_of(n * 512, 512), 512)
            o = contract_last(H[rows], Wgu[cols, :])
            done = 0
            for dz, dx, first, count in GROUPS[g]:
                O[dz, dx, first : first + count, cols] = o[done : done + count]
                done += count

    def backward(g):
        product(g)
        run(after.get(g, ()))

    def out_down(r):
        xsa[r] = O[r, 2].astype(BF16)
        c.send(f"d{r}", xsa.at[r], xd.at[r], {1: zp, 3: zm}[r])

    def out_far(r):
        total = O[r, 2]
        if r == 0:
            c.need("d1", "d3")
            total = total + xd[1].astype(F32) + xd[3].astype(F32)
        xsa[r] = total.astype(BF16)
        c.send(f"xa+{r}", xsa.at[r, :, L], xa.at[r // 2, 0], xp)
        c.send(f"xa-{r}", xsa.at[r, :, R], xa.at[r // 2, 1], xm)

    def out_pass(r):
        c.need(f"xa+{r}", f"xa-{r}")
        c.send(f"xd+{r}", xa.at[r // 2, 0], xd.at[r, :, L], xp)
        c.send(f"xd-{r}", xa.at[r // 2, 1], xd.at[r, :, R], xm)

    def out_near(r, dx, rows=(0, ROWS), halves=(0, 1)):
        k, sign, device = {1: (0, "+", xp), 3: (1, "-", xm)}[dx]
        at, to = slice(*rows), pl.ds(rows[0], rows[1] - rows[0])
        cols = pl.ds(halves[0] * HALF, len(halves) * HALF)
        xsb[r, k, at, cols] = O[r, dx, at, cols].astype(BF16)
        c.send(f"xb{sign}{r}_{rows[0]}_{halves[0]}", xsb.at[r, k, to, cols], xb.at[r, k, to, cols], device)

    def over_x(r, at, cols):
        near = O[r, 0, at, cols] + xb[r, 0, at, cols].astype(F32) + xb[r, 1, at, cols].astype(F32)
        return near + xd[r, at, cols].astype(F32) if r in (0, 2) else near

    def out_sum(r, rows=(0, ROWS), halves=(0, 1)):
        c.need(f"xb+{r}_0_0", f"xb-{r}_0_0")
        if r == 2:
            c.need("xd+2", "xd-2")
        at, to = slice(*rows), pl.ds(rows[0], rows[1] - rows[0])
        cols = pl.ds(halves[0] * HALF, len(halves) * HALF)
        zs[r - 1, at, cols] = over_x(r, at, cols).astype(BF16)
        if r == 2:
            c.send("z2+", zs.at[1, :, L], zt.at[0], zp)
            c.send("z2-", zs.at[1, :, R], zt.at[1], zm)
        else:
            name = f"z{r}_{rows[0]}_{halves[0]}"
            c.send(name, zs.at[r - 1, to, cols], zr.at[r - 1, to, cols], {1: zp, 3: zm}[r])

    def out_sum_far():
        c.need("z2+", "z2-")
        c.send("z2f+", zt.at[0], zr.at[1, :, L], zp)
        c.send("z2f-", zt.at[1], zr.at[1, :, R], zm)

    def out_final(first, rows):
        at = slice(first, first + rows)
        total = over_x(0, at, slice(0, WIDTH))
        for k in range(3):
            total += zr[k, at].astype(F32)
        out_ref[at] = total.astype(BF16)

    after = {
        1: ((out_near, 0, 1, (0, EARLY)), (out_near, 0, 3, (0, EARLY))),
        3: ((out_near, 1, 1), (out_near, 3, 3)),
        4: ((out_near, 1, 3), (out_near, 3, 1)),
        5: ((out_far, 2), (out_down, 1), (out_sum, 1, (0, EARLY)), (out_sum, 3, (0, EARLY))),
        6: ((out_down, 3), (out_near, 2, 1), (out_near, 2, 3)),
        7: ((out_far, 0),),
    }

    def run(events):
        for event, *args in events:
            event(*args)

    for n, (q, j) in enumerate(own):
        for k, (src, dst) in enumerate(pieces(q, j)):
            local(src, dst, weight_sems.at[3 * q + k])
    for copy in own_tokens:
        copy.wait()
    forward(0, 0, 1)
    reduce_far(0)
    forward(0, 1, 4)
    reduce_near(0)
    forward(1)
    reduce_far(1)
    relay_1()
    grads(0)
    forward(2)
    reduce_far(2)
    reduce_near(1)
    spread(0)
    reduce_near(2)
    grads(1)
    forward(3)
    reduce_far(3)
    relay_2()
    backward(0)
    spread(1)
    relay_3()
    for t in range(3, last):
        if t > 3:
            reduce_far(t)
        if t == 4:
            relay_4()
        grads(t - 1)
        backward(t - 2)
        reduce_near(t)
        if t + 1 in relays:
            relays[t + 1]()
        forward(t + 1)
        spread(t - 1)
    reduce_far(last)
    grads(last - 1)
    out_pass(2)
    backward(last - 2)
    reduce_near(last)
    spread(last - 1)
    grads(last)
    backward(last - 1)
    spread(last)
    out_sum(2)
    for h in (0, 1):
        product(last, 2 * h, 2)
        out_near(0, 1, (EARLY, ROWS), (h,))
        out_near(0, 3, (EARLY, ROWS), (h,))
        out_sum(1, (EARLY, ROWS), (h,))
        out_sum(3, (EARLY, ROWS), (h,))
        if h == 0:
            out_pass(0)
    out_sum_far()
    for copy in locals_:
        copy.wait_send()
    c.finish()
    out_final(0, ROWS // 2)
    out_final(ROWS // 2, ROWS // 2)


def shards(inputs, out_grad, gate_weight, up_weight, down_weight):
    return pl.pallas_call(
        kernel,
        out_shape=pltpu.VMEM((ROWS, WIDTH), BF16),
        in_specs=[pl.BlockSpec(memory_space=pl.ANY)] * 5,
        out_specs=pl.BlockSpec(memory_space=pltpu.VMEM),
        scratch_shapes=[
            pltpu.VMEM((4, 4, ROWS, WIDTH), BF16),
            pltpu.VMEM((4, 4, ROWS, WIDTH), BF16),
            pltpu.VMEM((WIDTH, 8 * Q), BF16),
            pltpu.VMEM((4 * Q, WIDTH), BF16),
            pltpu.VMEM((2, 4, TOP, 3 * Q), F32),
            pltpu.VMEM((4, 4, ROWS, WIDTH), F32),
            pltpu.VMEM((2, ALL, CUT), BF16),
            pltpu.VMEM((2, ALL, 3 * Q), BF16),
            pltpu.VMEM((ALL, 8 * Q), BF16),
            pltpu.VMEM((2, TOP, 3 * Q), BF16),
            pltpu.VMEM((2, 2, TOP, 3 * Q), BF16),
            pltpu.VMEM((4, ROWS, WIDTH), BF16),
            pltpu.VMEM((4, 2, ROWS, WIDTH), BF16),
            pltpu.VMEM((2, 2, ROWS, HALF), BF16),
            pltpu.VMEM((4, 2, ROWS, WIDTH), BF16),
            pltpu.VMEM((4, ROWS, WIDTH), BF16),
            pltpu.VMEM((3, ROWS, WIDTH), BF16),
            pltpu.VMEM((2, ROWS, HALF), BF16),
            pltpu.VMEM((3, ROWS, WIDTH), BF16),
            pltpu.SemaphoreType.DMA((SENDS,)),
            pltpu.SemaphoreType.DMA((RECVS,)),
            pltpu.SemaphoreType.DMA((2,)),
            pltpu.SemaphoreType.DMA((6,)),
            pltpu.SemaphoreType.DMA((12,)),
        ],
        compiler_params=pltpu.CompilerParams(
            collective_id=0, has_side_effects=True, vmem_limit_bytes=65_000_000
        ),
        name="swiglu_back",
    )(inputs, out_grad, gate_weight, up_weight, down_weight)


def solution(mesh):
    return jax.shard_map(
        shards,
        mesh=mesh,
        in_specs=(
            P(("gx", "gz"), "gy"),
            P(("gx", "gz"), "gy"),
            P("gy", ("gx", "gz")),
            P("gy", ("gx", "gz")),
            P(("gx", "gz"), "gy"),
        ),
        out_specs=P(("gx", "gz"), "gy"),
        check_vma=False,
    )
```

```python
import jax
import jax.numpy as jnp
from jax import lax
from jax.experimental import pallas as pl
from jax.experimental.pallas import tpu as pltpu
from jax.sharding import PartitionSpec as P

MESH = pl.DeviceIdType.MESH
F32 = jnp.float32
BF16 = jnp.bfloat16

ROWS = 80
WIDTH = 2048
HALF = WIDTH // 2
OWN = 512
Q = 256
CUT = 3 * Q // 2

GROUPS = (
    ((0, 0, 0, 80),),
    ((0, 1, 0, 48), (0, 3, 0, 48)),
    ((1, 0, 0, 48), (3, 0, 0, 48)),
    ((1, 1, 0, 80), (3, 3, 0, 80)),
    ((1, 3, 0, 80), (3, 1, 0, 80)),
    ((2, 2, 0, 80), (1, 2, 0, 80), (2, 1, 0, 48)),
    ((3, 2, 0, 80), (2, 3, 0, 80), (2, 1, 48, 32)),
    ((0, 2, 0, 80), (2, 0, 0, 80)),
    ((1, 0, 48, 32), (3, 0, 48, 32), (0, 1, 48, 32), (0, 3, 48, 32)),
)
EARLY = 48
SIZES = tuple(sum(rows for *_, rows in group) for group in GROUPS)
STARTS = tuple(sum(SIZES[:g]) for g in range(len(SIZES)))
TOP = max(SIZES)
ALL = sum(SIZES)


def contract_last(left, right):
    return lax.dot_general(
        left, right, (((1,), (1,)), ((), ())), preferred_element_type=F32
    )


class Copies:
    def __init__(self, send_sems, recv_sems):
        self.send_sems, self.recv_sems = send_sems, recv_sems
        self.made, self.sent, self.landed = {}, {}, set()
        self.keys, self.user, self.pairs = {}, {}, {}

    def send(self, name, src, dst, device, both=None):
        k = len(self.made) % SENDS
        for old in [old for old, at in self.sent.items() if at == k]:
            self.free(old)
        base = name if both is None else name.replace("+", "").replace("-", "")
        key = base[:2] + str(int(base[2:]) % 3) if base[:2] in OVER_Y else base
        r = self.keys.setdefault(key, len(self.keys))
        assert self.user.get(key, base) == base or self.user[key] in self.landed
        self.user[key] = base
        copy = pltpu.make_async_remote_copy(
            src_ref=src,
            dst_ref=dst,
            send_sem=self.send_sems.at[k],
            recv_sem=self.recv_sems.at[r],
            device_id=device,
            device_id_type=MESH,
        )
        self.made[name] = copy
        self.sent[name] = k
        if both is not None:
            self.pairs[name] = base, (both, both, self.recv_sems.at[r])
        copy.start()

    def need(self, *names):
        for name in names:
            base, pair = self.pairs.get(name, (name, None))
            if base not in self.landed:
                self.landed.add(base)
                if pair is None:
                    self.made[name].wait_recv()
                else:
                    pltpu.make_async_copy(*pair).wait()

    def free(self, *names):
        for name in names:
            if name in self.sent:
                del self.sent[name]
                self.made[name].wait_send()

    def finish(self):
        assert len(self.keys) == RECVS
        self.need(*self.made)
        self.free(*list(self.sent))


OVER_Y = ("ra", "rb", "ga", "gf")
SENDS = 28
RECVS = 76


def kernel(
    x_hbm, g_hbm, wg_hbm, wu_hbm, wd_hbm, out_ref,
    A, B, Wgu, Wd, S, O, ra, rb, H, sa, sb, xsa, xsb, xa, xb, xd, zs, zt, zr,
    send_sems, recv_sems, local_sems, weight_sends, weight_sems,
):
    gx, y, gz = lax.axis_index("gx"), lax.axis_index("gy"), lax.axis_index("gz")
    x = lax.div(gz, 2) * 2 + lax.div(gx, 4)
    z = lax.rem(gx, 4)
    core = lax.rem(gz, 2)

    def device(dx=0, dy=0, dz=0):
        nx, ny, nz = (lax.rem(p + d + 4, 4) for p, d in ((x, dx), (y, dy), (z, dz)))
        return {
            "gx": lax.rem(nx, 2) * 4 + nz,
            "gy": ny,
            "gz": lax.div(nx, 2) * 2 + core,
        }

    partner = {"gx": gx, "gy": y, "gz": gz + 1 - 2 * core}
    xp, xm = device(dx=1), device(dx=-1)
    yp, ym = device(dy=1), device(dy=-1)
    zp, zm = device(dz=1), device(dz=-1)

    barrier = pltpu.get_barrier_semaphore()
    peers = (partner, xp, xm, yp, ym, zp, zm)
    own_tokens = [
        pltpu.make_async_copy(src, ref.at[0, 0], local_sems.at[k])
        for k, (src, ref) in enumerate(((x_hbm, A), (g_hbm, B)))
    ]
    for copy in own_tokens:
        copy.start()
    for peer in peers:
        pl.semaphore_signal(barrier, inc=1, device_id=peer, device_id_type=MESH)
    pl.semaphore_wait(barrier, len(peers))

    c = Copies(send_sems, recv_sems)
    L, R = pl.ds(0, HALF), pl.ds(HALF, HALF)

    near = lax.rem(y + 2, 4)
    mine = 1 - jnp.abs(lax.div(near, 2) - core)
    lead = mine * lax.rem(near, 2)
    locals_ = []

    def local(src, dst, sem):
        copy = pltpu.make_async_copy(src, dst, sem)
        copy.start()
        return copy

    def pieces(q, j):
        wide, narrow = pl.multiple_of(q * 2 * Q, 2 * Q), pl.multiple_of(q * Q, Q)
        part = pl.ds(pl.multiple_of(j * Q, Q), Q)
        return (
            (wg_hbm.at[:, part], Wgu.at[:, pl.ds(wide, Q)]),
            (wu_hbm.at[:, part], Wgu.at[:, pl.ds(wide + Q, Q)]),
            (wd_hbm.at[part], Wd.at[pl.ds(narrow, Q)]),
        )

    own = [(2 * core + j, j) for j in (lead, 1 - lead)]
    for n, (q, j) in enumerate(own):
        for k, (src, dst) in enumerate(pieces(q, j)):
            copy = pltpu.make_async_remote_copy(
                src_ref=src,
                dst_ref=dst,
                send_sem=weight_sends.at[3 * n + k],
                recv_sem=weight_sems.at[3 * q + k],
                device_id=partner,
                device_id_type=MESH,
            )
            copy.start()
            locals_.append(copy)

    def own_over_x(name, hbm, ref, rows):
        c.send(name.replace("@", "+"), hbm.at[rows], ref.at[0, 3, rows], xp)
        c.send(name.replace("@", "-"), hbm.at[rows], ref.at[0, 1, rows], xm)

    def own_over_z(name, hbm, ref, rows):
        c.send(name.replace("@", "+"), hbm.at[rows], ref.at[3, 0, rows], zp)
        c.send(name.replace("@", "-"), hbm.at[rows], ref.at[1, 0, rows], zm)

    ahead, behind = pl.ds(0, EARLY), pl.ds(EARLY, ROWS - EARLY)
    own_over_x("Ax@", x_hbm, A, ahead)
    own_over_z("Bz@", g_hbm, B, ahead)
    own_over_x("Bx@0", g_hbm, B, ahead)
    own_over_z("Az@0", x_hbm, A, ahead)
    own_over_x("Ax@b", x_hbm, A, behind)
    own_over_z("Bz@b", g_hbm, B, behind)

    def need_weights(q):
        for k, (src, dst) in enumerate(pieces(q, 0)):
            pltpu.make_async_copy(src, dst, weight_sems.at[3 * q + k]).wait()

    def a_over_z(dx):
        c.send(f"Az+{dx}", A.at[0, dx], A.at[3, dx], zp)
        c.send(f"Az-{dx}", A.at[0, dx], A.at[1, dx], zm)

    def a_over_z_far(dx):
        c.need(f"Az+{dx}", f"Az-{dx}")
        if dx == 0:
            c.need("Az+0b", "Az-0b")
        c.send(f"Azf+{dx}", A.at[3, dx, :, L], A.at[2, dx, :, L], zp, A.at[2, dx])
        c.send(f"Azf-{dx}", A.at[1, dx, :, R], A.at[2, dx, :, R], zm, A.at[2, dx])

    def b_over_x(dz):
        c.send(f"Bx+{dz}", B.at[dz, 0], B.at[dz, 3], xp)
        c.send(f"Bx-{dz}", B.at[dz, 0], B.at[dz, 1], xm)

    def b_over_x_far(dz):
        c.need(f"Bx+{dz}", f"Bx-{dz}")
        if dz == 0:
            c.need("Bx+0b", "Bx-0b")
        c.send(f"Bxf+{dz}", B.at[dz, 3, :, L], B.at[dz, 2, :, L], xp, B.at[dz, 2])
        c.send(f"Bxf-{dz}", B.at[dz, 1, :, R], B.at[dz, 2, :, R], xm, B.at[dz, 2])

    def relay_1():
        c.need("Ax+", "Ax-", "Ax+b", "Ax-b")
        c.send("Az-1", A.at[0, 1], A.at[1, 1], zm)
        c.send("Az+3", A.at[0, 3], A.at[3, 3], zp)
        c.need("Bz+", "Bz-", "Bz+b", "Bz-b")
        c.send("Bx-1", B.at[1, 0], B.at[1, 1], xm)
        c.send("Bx+3", B.at[3, 0], B.at[3, 3], xp)
        c.send("Axf+", A.at[0, 3, :, L], A.at[0, 2, :, L], xp, A.at[0, 2])
        c.send("Axf-", A.at[0, 1, :, R], A.at[0, 2, :, R], xm, A.at[0, 2])
        c.send("Bzf+", B.at[3, 0, :, L], B.at[2, 0, :, L], zp, B.at[2, 0])
        c.send("Bzf-", B.at[1, 0, :, R], B.at[2, 0, :, R], zm, B.at[2, 0])
        c.send("Az+1", A.at[0, 1], A.at[3, 1], zp)
        c.send("Az-3", A.at[0, 3], A.at[1, 3], zm)
        c.send("Bx+1", B.at[1, 0], B.at[1, 3], xp)
        c.send("Bx-3", B.at[3, 0], B.at[3, 1], xm)

    def relay_2():
        c.need("Bzf+", "Bzf-")
        b_over_x(2)
        c.need("Axf+", "Axf-")
        a_over_z(2)

    def relay_3():
        b_over_x_far(1)
        a_over_z_far(1)

    def relay_4():
        a_over_z_far(2)
        b_over_x_far(2)
        a_over_z_far(3)
        b_over_x_far(3)
        own_over_z("Az@0b", x_hbm, A, behind)

    def relay_5():
        own_over_x("Bx@0b", g_hbm, B, behind)

    def relay_6():
        a_over_z_far(0)
        b_over_x_far(0)

    relays = {5: relay_5, 6: relay_6}

    def need_tokens(g):
        for dz, dx, first, _ in GROUPS[g]:
            late = first >= EARLY
            if dz == 0:
                c.need(*{0: (), 1: ("Ax-", "Bx-0"), 2: ("Axf+", "Axf-", "Bxf+0", "Bxf-0"), 3: ("Ax+", "Bx+0")}[dx])
                if late:
                    c.need(*{0: (), 1: ("Ax-b", "Bx-0b"), 2: (), 3: ("Ax+b", "Bx+0b")}[dx])
                continue
            c.need(*{1: (f"Az-{dx}",), 2: (f"Azf+{dx}", f"Azf-{dx}"), 3: (f"Az+{dx}",)}[dz])
            if dx == 0:
                c.need(*{1: ("Bz-",), 2: ("Bzf+", "Bzf-"), 3: ("Bz+",)}[dz])
                if late:
                    c.need(*{1: ("Az-0b", "Bz-b"), 2: (), 3: ("Az+0b", "Bz+b")}[dz])
            else:
                c.need(*{1: (f"Bx-{dz}",), 2: (f"Bxf+{dz}", f"Bxf-{dz}"), 3: (f"Bx+{dz}",)}[dx])

    def rows_of(ref, g):
        parts = [ref[dz, dx, first : first + rows] for dz, dx, first, rows in GROUPS[g]]
        return parts[0] if len(parts) == 1 else jnp.concatenate(parts, axis=0)

    def quarter(k):
        return lax.rem(y + k, 4)

    def forward(g, start=0, stop=4):
        m = SIZES[g]
        need_tokens(g)

        @pl.loop(start, stop)
        def _(k):
            q = lax.rem(y + 2 + k, 4)
            if g == 0:
                need_weights(q)
            w = Wgu[:, pl.ds(pl.multiple_of(q * 2 * Q, 2 * Q), 2 * Q)]
            S[g % 2, k, 0:m, 0 : 2 * Q] = jnp.dot(rows_of(A, g), w, preferred_element_type=F32)
            d = Wd[pl.ds(pl.multiple_of(q * Q, Q), Q), :]
            S[g % 2, k, 0:m, 2 * Q : 3 * Q] = contract_last(rows_of(B, g), d)

    def reduce_far(g):
        s, m = g % 2, SIZES[g]
        at = pl.ds(STARTS[g], m)
        if g >= 2:
            c.free(f"ra+{g - 2}", f"ra-{g - 2}")
        sa[s, 0:m] = S[s, 0, 0:m].astype(BF16)
        c.send(f"ra+{g}", sa.at[s, pl.ds(0, m), pl.ds(0, CUT)], ra.at[0, at], yp, ra.at[:, at])
        c.send(f"ra-{g}", sa.at[s, pl.ds(0, m), pl.ds(CUT, CUT)], ra.at[1, at], ym, ra.at[:, at])

    def reduce_near(g):
        s, m = g % 2, SIZES[g]
        at, rows = slice(STARTS[g], STARTS[g] + m), pl.ds(STARTS[g], m)
        if g >= 2:
            c.free(f"rb+{g - 2}", f"rb-{g - 2}")
        c.need(f"ra+{g}", f"ra-{g}")
        sb[s, 0, 0:m, 0:CUT] = (S[s, 3, 0:m, 0:CUT] + ra[0, at].astype(F32)).astype(BF16)
        sb[s, 0, 0:m, CUT:] = S[s, 3, 0:m, CUT:].astype(BF16)
        c.send(f"rb+{g}", sb.at[s, 0, pl.ds(0, m)], rb.at[0, rows], yp, rb.at[:, rows])
        sb[s, 1, 0:m, 0:CUT] = S[s, 1, 0:m, 0:CUT].astype(BF16)
        sb[s, 1, 0:m, CUT:] = (S[s, 1, 0:m, CUT:] + ra[1, at].astype(F32)).astype(BF16)
        c.send(f"rb-{g}", sb.at[s, 1, pl.ds(0, m)], rb.at[1, rows], ym, rb.at[:, rows])

    last = len(GROUPS) - 1

    def grads(g):
        s, m = g % 2, SIZES[g]
        rows = pl.ds(STARTS[g], m)
        c.need(f"rb+{g}", f"rb-{g}")

        def total(at):
            cols = pl.ds(at, Q)
            return S[s, 2, 0:m, cols] + rb[0, rows, cols].astype(F32) + rb[1, rows, cols].astype(F32)

        gate, upper, hidden_grad = total(0), total(Q), total(2 * Q)
        logistic = 1.0 / (1.0 + jnp.exp(-gate))
        scaled = hidden_grad * logistic
        at = pl.multiple_of(y * (2 * Q), 2 * Q)
        H[rows, pl.ds(at, Q)] = (scaled * upper * (1.0 + gate * (1.0 - logistic))).astype(BF16)
        H[rows, pl.ds(at + Q, Q)] = (scaled * gate).astype(BF16)
        own = H.at[rows, pl.ds(at, 2 * Q)]
        c.send(f"ga+{g}", own, own, yp, H.at[rows, pl.ds(0, 4 * Q)])
        c.send(f"ga-{g}", own, own, ym, H.at[rows, pl.ds(0, 4 * Q)])

    def spread(g):
        rows = pl.ds(STARTS[g], SIZES[g])
        c.need(f"ga+{g}", f"ga-{g}")
        at = pl.multiple_of(quarter(3) * (2 * Q), 2 * Q)
        part = H.at[rows, pl.ds(at, Q)]
        c.send(f"gf+{g}", part, part, yp, H.at[rows, pl.ds(0, 2 * Q)])
        at = pl.multiple_of(quarter(1) * (2 * Q), 2 * Q)
        part = H.at[rows, pl.ds(at + Q, Q)]
        c.send(f"gf-{g}", part, part, ym, H.at[rows, pl.ds(0, 2 * Q)])

    def product(g, start=0, steps=4):
        rows = slice(STARTS[g], STARTS[g] + SIZES[g])
        c.need(f"gf+{g}", f"gf-{g}")

        @pl.loop(start, start + steps)
        def _(n):
            cols = pl.ds(pl.multiple_of(n * 512, 512), 512)
            o = contract_last(H[rows], Wgu[cols, :])
            done = 0
            for dz, dx, first, count in GROUPS[g]:
                O[dz, dx, first : first + count, cols] = o[done : done + count]
                done += count

    def backward(g):
        product(g)
        run(after.get(g, ()))

    def out_down(r):
        xsa[r] = O[r, 2].astype(BF16)
        c.send(f"d{r}", xsa.at[r], xd.at[r], {1: zp, 3: zm}[r])

    def out_far(r):
        total = O[r, 2]
        if r == 0:
            c.need("d1", "d3")
            total = total + xd[1].astype(F32) + xd[3].astype(F32)
        xsa[r] = total.astype(BF16)
        c.send(f"xa+{r}", xsa.at[r, :, L], xa.at[r // 2, 0], xp, xa.at[r // 2])
        c.send(f"xa-{r}", xsa.at[r, :, R], xa.at[r // 2, 1], xm, xa.at[r // 2])

    def out_pass(r):
        c.need(f"xa+{r}", f"xa-{r}")
        c.send(f"xd+{r}", xa.at[r // 2, 0], xd.at[r, :, L], xp, xd.at[r])
        c.send(f"xd-{r}", xa.at[r // 2, 1], xd.at[r, :, R], xm, xd.at[r])

    def out_near(r, dx, rows=(0, ROWS), halves=(0, 1)):
        k, sign, device = {1: (0, "+", xp), 3: (1, "-", xm)}[dx]
        at, to = slice(*rows), pl.ds(rows[0], rows[1] - rows[0])
        cols = pl.ds(halves[0] * HALF, len(halves) * HALF)
        xsb[r, k, at, cols] = O[r, dx, at, cols].astype(BF16)
        c.send(f"xb{sign}{r}_{rows[0]}_{halves[0]}", xsb.at[r, k, to, cols], xb.at[r, k, to, cols], device)

    def over_x(r, at, cols):
        near = O[r, 0, at, cols] + xb[r, 0, at, cols].astype(F32) + xb[r, 1, at, cols].astype(F32)
        return near + xd[r, at, cols].astype(F32) if r in (0, 2) else near

    def out_sum(r, rows=(0, ROWS), halves=(0, 1)):
        c.need(f"xb+{r}_0_0", f"xb-{r}_0_0")
        if r == 2:
            c.need("xd+2", "xd-2")
        at, to = slice(*rows), pl.ds(rows[0], rows[1] - rows[0])
        cols = pl.ds(halves[0] * HALF, len(halves) * HALF)
        zs[r - 1, at, cols] = over_x(r, at, cols).astype(BF16)
        if r == 2:
            c.send("z2+", zs.at[1, :, L], zt.at[0], zp, zt)
            c.send("z2-", zs.at[1, :, R], zt.at[1], zm, zt)
        else:
            name = f"z{r}_{rows[0]}_{halves[0]}"
            c.send(name, zs.at[r - 1, to, cols], zr.at[r - 1, to, cols], {1: zp, 3: zm}[r])

    def out_sum_far():
        c.need("z2+", "z2-")
        c.send("z2f+", zt.at[0], zr.at[1, :, L], zp, zr.at[1])
        c.send("z2f-", zt.at[1], zr.at[1, :, R], zm, zr.at[1])

    def out_final(first, rows):
        at = slice(first, first + rows)
        total = over_x(0, at, slice(0, WIDTH))
        for k in range(3):
            total += zr[k, at].astype(F32)
        out_ref[at] = total.astype(BF16)

    after = {
        1: ((out_near, 0, 1, (0, EARLY)), (out_near, 0, 3, (0, EARLY))),
        3: ((out_near, 1, 1), (out_near, 3, 3)),
        4: ((out_near, 1, 3), (out_near, 3, 1)),
        5: ((out_far, 2), (out_down, 1), (out_sum, 1, (0, EARLY)), (out_sum, 3, (0, EARLY))),
        6: ((out_down, 3), (out_near, 2, 1), (out_near, 2, 3)),
        7: ((out_far, 0),),
    }

    def run(events):
        for event, *args in events:
            event(*args)

    for n, (q, j) in enumerate(own):
        for k, (src, dst) in enumerate(pieces(q, j)):
            local(src, dst, weight_sems.at[3 * q + k])
    for copy in own_tokens:
        copy.wait()
    forward(0, 0, 1)
    reduce_far(0)
    forward(0, 1, 4)
    reduce_near(0)
    forward(1)
    reduce_far(1)
    relay_1()
    grads(0)
    forward(2)
    reduce_far(2)
    reduce_near(1)
    spread(0)
    reduce_near(2)
    grads(1)
    forward(3)
    reduce_far(3)
    relay_2()
    backward(0)
    spread(1)
    relay_3()
    for t in range(3, last):
        if t > 3:
            reduce_far(t)
        if t == 4:
            relay_4()
        grads(t - 1)
        backward(t - 2)
        reduce_near(t)
        if t + 1 in relays:
            relays[t + 1]()
        forward(t + 1)
        spread(t - 1)
    reduce_far(last)
    grads(last - 1)
    out_pass(2)
    backward(last - 2)
    reduce_near(last)
    spread(last - 1)
    grads(last)
    backward(last - 1)
    spread(last)
    out_sum(2)

    def out_last(h):
        out_near(0, 1, (EARLY, ROWS), (h,))
        out_near(0, 3, (EARLY, ROWS), (h,))
        out_sum(1, (EARLY, ROWS), (h,))
        out_sum(3, (EARLY, ROWS), (h,))

    product(last, 0, 2)
    out_last(0)
    out_pass(0)
    product(last, 2, 1)
    out_sum_far()
    product(last, 3, 1)
    out_last(1)
    for copy in locals_:
        copy.wait_send()
    c.finish()
    out_final(0, ROWS // 2)
    out_final(ROWS // 2, ROWS // 2)


def shards(inputs, out_grad, gate_weight, up_weight, down_weight):
    return pl.pallas_call(
        kernel,
        out_shape=pltpu.VMEM((ROWS, WIDTH), BF16),
        in_specs=[pl.BlockSpec(memory_space=pl.ANY)] * 5,
        out_specs=pl.BlockSpec(memory_space=pltpu.VMEM),
        scratch_shapes=[
            pltpu.VMEM((4, 4, ROWS, WIDTH), BF16),
            pltpu.VMEM((4, 4, ROWS, WIDTH), BF16),
            pltpu.VMEM((WIDTH, 8 * Q), BF16),
            pltpu.VMEM((4 * Q, WIDTH), BF16),
            pltpu.VMEM((2, 4, TOP, 3 * Q), F32),
            pltpu.VMEM((4, 4, ROWS, WIDTH), F32),
            pltpu.VMEM((2, ALL, CUT), BF16),
            pltpu.VMEM((2, ALL, 3 * Q), BF16),
            pltpu.VMEM((ALL, 8 * Q), BF16),
            pltpu.VMEM((2, TOP, 3 * Q), BF16),
            pltpu.VMEM((2, 2, TOP, 3 * Q), BF16),
            pltpu.VMEM((4, ROWS, WIDTH), BF16),
            pltpu.VMEM((4, 2, ROWS, WIDTH), BF16),
            pltpu.VMEM((2, 2, ROWS, HALF), BF16),
            pltpu.VMEM((4, 2, ROWS, WIDTH), BF16),
            pltpu.VMEM((4, ROWS, WIDTH), BF16),
            pltpu.VMEM((3, ROWS, WIDTH), BF16),
            pltpu.VMEM((2, ROWS, HALF), BF16),
            pltpu.VMEM((3, ROWS, WIDTH), BF16),
            pltpu.SemaphoreType.DMA((SENDS,)),
            pltpu.SemaphoreType.DMA((RECVS,)),
            pltpu.SemaphoreType.DMA((2,)),
            pltpu.SemaphoreType.DMA((6,)),
            pltpu.SemaphoreType.DMA((12,)),
        ],
        compiler_params=pltpu.CompilerParams(
            collective_id=0, has_side_effects=True, vmem_limit_bytes=65_000_000
        ),
        name="swiglu_back",
    )(inputs, out_grad, gate_weight, up_weight, down_weight)


def solution(mesh):
    return jax.shard_map(
        shards,
        mesh=mesh,
        in_specs=(
            P(("gx", "gz"), "gy"),
            P(("gx", "gz"), "gy"),
            P("gy", ("gx", "gz")),
            P("gy", ("gx", "gz")),
            P(("gx", "gz"), "gy"),
        ),
        out_specs=P(("gx", "gz"), "gy"),
        check_vma=False,
    )
```

```python
import jax
import jax.numpy as jnp
from jax import lax
from jax.experimental import pallas as pl
from jax.experimental.pallas import tpu as pltpu
from jax.sharding import PartitionSpec as P

MESH = pl.DeviceIdType.MESH
F32 = jnp.float32
BF16 = jnp.bfloat16

ROWS = 80
WIDTH = 2048
HALF = WIDTH // 2
OWN = 512
Q = 256
CUT = 3 * Q // 2

GROUPS = (
    ((0, 0, 0, 80),),
    ((0, 1, 0, 48), (0, 3, 0, 48)),
    ((1, 0, 0, 48), (3, 0, 0, 48)),
    ((1, 1, 0, 80), (3, 3, 0, 80)),
    ((1, 3, 0, 80), (3, 1, 0, 80)),
    ((2, 2, 0, 80), (1, 2, 0, 80), (2, 1, 0, 48)),
    ((3, 2, 0, 80), (2, 3, 0, 80), (2, 1, 48, 32)),
    ((0, 2, 0, 80), (2, 0, 0, 80)),
    ((1, 0, 48, 32), (3, 0, 48, 32), (0, 1, 48, 32), (0, 3, 48, 32)),
)
EARLY = 48
SIZES = tuple(sum(rows for *_, rows in group) for group in GROUPS)
STARTS = tuple(sum(SIZES[:g]) for g in range(len(SIZES)))
TOP = max(SIZES)
ALL = sum(SIZES)


def contract_last(left, right):
    return lax.dot_general(
        left, right, (((1,), (1,)), ((), ())), preferred_element_type=F32
    )


class Copies:
    def __init__(self, send_sems, recv_sems):
        self.send_sems, self.recv_sems = send_sems, recv_sems
        self.made, self.sent, self.landed = {}, {}, set()
        self.keys, self.user, self.pairs = {}, {}, {}

    def send(self, name, src, dst, device, both=None):
        k = len(self.made) % SENDS
        for old in [old for old, at in self.sent.items() if at == k]:
            self.free(old)
        base = name if both is None else name.replace("+", "").replace("-", "")
        key = base[:2] + str(int(base[2:]) % 3) if base[:2] in OVER_Y else base
        r = self.keys.setdefault(key, len(self.keys))
        assert self.user.get(key, base) == base or self.user[key] in self.landed
        self.user[key] = base
        copy = pltpu.make_async_remote_copy(
            src_ref=src,
            dst_ref=dst,
            send_sem=self.send_sems.at[k],
            recv_sem=self.recv_sems.at[r],
            device_id=device,
            device_id_type=MESH,
        )
        self.made[name] = copy
        self.sent[name] = k
        if both is not None:
            self.pairs[name] = base, (both, both, self.recv_sems.at[r])
        copy.start()

    def need(self, *names):
        for name in names:
            base, pair = self.pairs.get(name, (name, None))
            if base not in self.landed:
                self.landed.add(base)
                if pair is None:
                    self.made[name].wait_recv()
                else:
                    pltpu.make_async_copy(*pair).wait()

    def free(self, *names):
        for name in names:
            if name in self.sent:
                del self.sent[name]
                self.made[name].wait_send()

    def finish(self):
        assert len(self.keys) == RECVS
        self.need(*self.made)
        self.free(*list(self.sent))


OVER_Y = ("ra", "rb", "ga", "gf")
SENDS = 28
RECVS = 80


def kernel(
    x_hbm, g_hbm, wg_hbm, wu_hbm, wd_hbm, out_ref,
    A, B, Wgu, Wd, S, O, ra, rb, H, sa, sb, xsa, xsb, xa, xb, xd, zs, zt, zr,
    send_sems, recv_sems, local_sems, weight_sends, weight_sems,
):
    gx, y, gz = lax.axis_index("gx"), lax.axis_index("gy"), lax.axis_index("gz")
    x = lax.div(gz, 2) * 2 + lax.div(gx, 4)
    z = lax.rem(gx, 4)
    core = lax.rem(gz, 2)

    def device(dx=0, dy=0, dz=0):
        nx, ny, nz = (lax.rem(p + d + 4, 4) for p, d in ((x, dx), (y, dy), (z, dz)))
        return {
            "gx": lax.rem(nx, 2) * 4 + nz,
            "gy": ny,
            "gz": lax.div(nx, 2) * 2 + core,
        }

    partner = {"gx": gx, "gy": y, "gz": gz + 1 - 2 * core}
    xp, xm = device(dx=1), device(dx=-1)
    yp, ym = device(dy=1), device(dy=-1)
    zp, zm = device(dz=1), device(dz=-1)

    barrier = pltpu.get_barrier_semaphore()
    peers = (partner, xp, xm, yp, ym, zp, zm)
    own_tokens = [
        pltpu.make_async_copy(src, ref.at[0, 0], local_sems.at[k])
        for k, (src, ref) in enumerate(((x_hbm, A), (g_hbm, B)))
    ]
    for copy in own_tokens:
        copy.start()
    for peer in peers:
        pl.semaphore_signal(barrier, inc=1, device_id=peer, device_id_type=MESH)
    pl.semaphore_wait(barrier, len(peers))

    c = Copies(send_sems, recv_sems)
    L, R = pl.ds(0, HALF), pl.ds(HALF, HALF)

    near = lax.rem(y + 2, 4)
    mine = 1 - jnp.abs(lax.div(near, 2) - core)
    lead = mine * lax.rem(near, 2)
    locals_ = []

    def local(src, dst, sem):
        copy = pltpu.make_async_copy(src, dst, sem)
        copy.start()
        return copy

    def pieces(q, j):
        wide, narrow = pl.multiple_of(q * 2 * Q, 2 * Q), pl.multiple_of(q * Q, Q)
        part = pl.ds(pl.multiple_of(j * Q, Q), Q)
        return (
            (wg_hbm.at[:, part], Wgu.at[:, pl.ds(wide, Q)]),
            (wu_hbm.at[:, part], Wgu.at[:, pl.ds(wide + Q, Q)]),
            (wd_hbm.at[part], Wd.at[pl.ds(narrow, Q)]),
        )

    own = [(2 * core + j, j) for j in (lead, 1 - lead)]
    for n, (q, j) in enumerate(own):
        for k, (src, dst) in enumerate(pieces(q, j)):
            copy = pltpu.make_async_remote_copy(
                src_ref=src,
                dst_ref=dst,
                send_sem=weight_sends.at[3 * n + k],
                recv_sem=weight_sems.at[3 * q + k],
                device_id=partner,
                device_id_type=MESH,
            )
            copy.start()
            locals_.append(copy)

    def own_over_x(name, hbm, ref, rows):
        c.send(name.replace("@", "+"), hbm.at[rows], ref.at[0, 3, rows], xp)
        c.send(name.replace("@", "-"), hbm.at[rows], ref.at[0, 1, rows], xm)

    def own_over_z(name, hbm, ref, rows):
        c.send(name.replace("@", "+"), hbm.at[rows], ref.at[3, 0, rows], zp)
        c.send(name.replace("@", "-"), hbm.at[rows], ref.at[1, 0, rows], zm)

    ahead, behind = pl.ds(0, EARLY), pl.ds(EARLY, ROWS - EARLY)
    own_over_x("Ax@", x_hbm, A, ahead)
    own_over_z("Bz@", g_hbm, B, ahead)
    own_over_x("Bx@0", g_hbm, B, ahead)
    own_over_z("Az@0", x_hbm, A, ahead)
    own_over_x("Ax@b", x_hbm, A, behind)
    own_over_z("Bz@b", g_hbm, B, behind)

    def need_weights(q):
        for k, (src, dst) in enumerate(pieces(q, 0)):
            pltpu.make_async_copy(src, dst, weight_sems.at[3 * q + k]).wait()

    def a_over_z(dx):
        c.send(f"Az+{dx}", A.at[0, dx], A.at[3, dx], zp)
        c.send(f"Az-{dx}", A.at[0, dx], A.at[1, dx], zm)

    def whole(*names):
        for name in names:
            c.need(name)
            if name + "b" in c.made:
                c.need(name + "b")

    def a_over_z_far(dx):
        whole(f"Az+{dx}", f"Az-{dx}")
        c.send(f"Azf+{dx}", A.at[3, dx, :, L], A.at[2, dx, :, L], zp, A.at[2, dx])
        c.send(f"Azf-{dx}", A.at[1, dx, :, R], A.at[2, dx, :, R], zm, A.at[2, dx])

    def b_over_x(dz):
        c.send(f"Bx+{dz}", B.at[dz, 0], B.at[dz, 3], xp)
        c.send(f"Bx-{dz}", B.at[dz, 0], B.at[dz, 1], xm)

    def b_over_x_far(dz):
        whole(f"Bx+{dz}", f"Bx-{dz}")
        c.send(f"Bxf+{dz}", B.at[dz, 3, :, L], B.at[dz, 2, :, L], xp, B.at[dz, 2])
        c.send(f"Bxf-{dz}", B.at[dz, 1, :, R], B.at[dz, 2, :, R], xm, B.at[dz, 2])

    def relay_first(piece, rows):
        c.need(f"Ax+{piece}", f"Ax-{piece}")
        c.send(f"Az-1{piece}", A.at[0, 1, rows], A.at[1, 1, rows], zm)
        c.send(f"Az+3{piece}", A.at[0, 3, rows], A.at[3, 3, rows], zp)
        c.need(f"Bz+{piece}", f"Bz-{piece}")
        c.send(f"Bx-1{piece}", B.at[1, 0, rows], B.at[1, 1, rows], xm)
        c.send(f"Bx+3{piece}", B.at[3, 0, rows], B.at[3, 3, rows], xp)

    def relay_1():
        c.send("Axf+", A.at[0, 3, :, L], A.at[0, 2, :, L], xp, A.at[0, 2])
        c.send("Axf-", A.at[0, 1, :, R], A.at[0, 2, :, R], xm, A.at[0, 2])
        c.send("Bzf+", B.at[3, 0, :, L], B.at[2, 0, :, L], zp, B.at[2, 0])
        c.send("Bzf-", B.at[1, 0, :, R], B.at[2, 0, :, R], zm, B.at[2, 0])
        c.send("Az+1", A.at[0, 1], A.at[3, 1], zp)
        c.send("Az-3", A.at[0, 3], A.at[1, 3], zm)
        c.send("Bx+1", B.at[1, 0], B.at[1, 3], xp)
        c.send("Bx-3", B.at[3, 0], B.at[3, 1], xm)

    def relay_2():
        c.need("Bzf+", "Bzf-")
        b_over_x(2)
        c.need("Axf+", "Axf-")
        a_over_z(2)

    def relay_3():
        b_over_x_far(1)
        a_over_z_far(1)

    def relay_4():
        a_over_z_far(2)
        b_over_x_far(2)
        a_over_z_far(3)
        b_over_x_far(3)
        own_over_z("Az@0b", x_hbm, A, behind)

    def relay_5():
        own_over_x("Bx@0b", g_hbm, B, behind)

    def relay_6():
        a_over_z_far(0)
        b_over_x_far(0)

    relays = {5: relay_5, 6: relay_6}

    def need_tokens(g):
        for dz, dx, first, _ in GROUPS[g]:
            late = first >= EARLY
            if dz == 0:
                c.need(*{0: (), 1: ("Ax-", "Bx-0"), 2: ("Axf+", "Axf-", "Bxf+0", "Bxf-0"), 3: ("Ax+", "Bx+0")}[dx])
                if late:
                    c.need(*{0: (), 1: ("Ax-b", "Bx-0b"), 2: (), 3: ("Ax+b", "Bx+0b")}[dx])
                continue
            need = c.need if dx == 0 else whole
            need(*{1: (f"Az-{dx}",), 2: (f"Azf+{dx}", f"Azf-{dx}"), 3: (f"Az+{dx}",)}[dz])
            if dx == 0:
                c.need(*{1: ("Bz-",), 2: ("Bzf+", "Bzf-"), 3: ("Bz+",)}[dz])
                if late:
                    c.need(*{1: ("Az-0b", "Bz-b"), 2: (), 3: ("Az+0b", "Bz+b")}[dz])
            else:
                whole(*{1: (f"Bx-{dz}",), 2: (f"Bxf+{dz}", f"Bxf-{dz}"), 3: (f"Bx+{dz}",)}[dx])

    def rows_of(ref, g):
        parts = [ref[dz, dx, first : first + rows] for dz, dx, first, rows in GROUPS[g]]
        return parts[0] if len(parts) == 1 else jnp.concatenate(parts, axis=0)

    def quarter(k):
        return lax.rem(y + k, 4)

    def forward(g, start=0, stop=4):
        m = SIZES[g]
        need_tokens(g)

        @pl.loop(start, stop)
        def _(k):
            q = lax.rem(y + 2 + k, 4)
            if g == 0:
                need_weights(q)
            w = Wgu[:, pl.ds(pl.multiple_of(q * 2 * Q, 2 * Q), 2 * Q)]
            S[g % 3, k, 0:m, 0 : 2 * Q] = jnp.dot(rows_of(A, g), w, preferred_element_type=F32)
            d = Wd[pl.ds(pl.multiple_of(q * Q, Q), Q), :]
            S[g % 3, k, 0:m, 2 * Q : 3 * Q] = contract_last(rows_of(B, g), d)

    def reduce_far(g):
        s, v, m = g % 2, g % 3, SIZES[g]
        at = pl.ds(STARTS[g], m)
        if g >= 2:
            c.free(f"ra+{g - 2}", f"ra-{g - 2}")
        sa[s, 0:m] = S[v, 0, 0:m].astype(BF16)
        c.send(f"ra+{g}", sa.at[s, pl.ds(0, m), pl.ds(0, CUT)], ra.at[0, at], yp, ra.at[:, at])
        c.send(f"ra-{g}", sa.at[s, pl.ds(0, m), pl.ds(CUT, CUT)], ra.at[1, at], ym, ra.at[:, at])

    def reduce_near(g):
        s, v, m = g % 2, g % 3, SIZES[g]
        at, rows = slice(STARTS[g], STARTS[g] + m), pl.ds(STARTS[g], m)
        if g >= 2:
            c.free(f"rb+{g - 2}", f"rb-{g - 2}")
        c.need(f"ra+{g}", f"ra-{g}")
        sb[s, 0, 0:m, 0:CUT] = (S[v, 3, 0:m, 0:CUT] + ra[0, at].astype(F32)).astype(BF16)
        sb[s, 0, 0:m, CUT:] = S[v, 3, 0:m, CUT:].astype(BF16)
        c.send(f"rb+{g}", sb.at[s, 0, pl.ds(0, m)], rb.at[0, rows], yp, rb.at[:, rows])
        sb[s, 1, 0:m, 0:CUT] = S[v, 1, 0:m, 0:CUT].astype(BF16)
        sb[s, 1, 0:m, CUT:] = (S[v, 1, 0:m, CUT:] + ra[1, at].astype(F32)).astype(BF16)
        c.send(f"rb-{g}", sb.at[s, 1, pl.ds(0, m)], rb.at[1, rows], ym, rb.at[:, rows])

    last = len(GROUPS) - 1

    def grads(g):
        v, m = g % 3, SIZES[g]
        rows = pl.ds(STARTS[g], m)
        c.need(f"rb+{g}", f"rb-{g}")

        def total(at):
            cols = pl.ds(at, Q)
            return S[v, 2, 0:m, cols] + rb[0, rows, cols].astype(F32) + rb[1, rows, cols].astype(F32)

        gate, upper, hidden_grad = total(0), total(Q), total(2 * Q)
        logistic = 1.0 / (1.0 + jnp.exp(-gate))
        scaled = hidden_grad * logistic
        at = pl.multiple_of(y * (2 * Q), 2 * Q)
        H[rows, pl.ds(at, Q)] = (scaled * upper * (1.0 + gate * (1.0 - logistic))).astype(BF16)
        H[rows, pl.ds(at + Q, Q)] = (scaled * gate).astype(BF16)
        own = H.at[rows, pl.ds(at, 2 * Q)]
        c.send(f"ga+{g}", own, own, yp, H.at[rows, pl.ds(0, 4 * Q)])
        c.send(f"ga-{g}", own, own, ym, H.at[rows, pl.ds(0, 4 * Q)])

    def spread(g):
        rows = pl.ds(STARTS[g], SIZES[g])
        c.need(f"ga+{g}", f"ga-{g}")
        at = pl.multiple_of(quarter(3) * (2 * Q), 2 * Q)
        part = H.at[rows, pl.ds(at, Q)]
        c.send(f"gf+{g}", part, part, yp, H.at[rows, pl.ds(0, 2 * Q)])
        at = pl.multiple_of(quarter(1) * (2 * Q), 2 * Q)
        part = H.at[rows, pl.ds(at + Q, Q)]
        c.send(f"gf-{g}", part, part, ym, H.at[rows, pl.ds(0, 2 * Q)])

    def product(g, start=0, steps=4):
        rows = slice(STARTS[g], STARTS[g] + SIZES[g])
        c.need(f"gf+{g}", f"gf-{g}")

        @pl.loop(start, start + steps)
        def _(n):
            cols = pl.ds(pl.multiple_of(n * 512, 512), 512)
            o = contract_last(H[rows], Wgu[cols, :])
            done = 0
            for dz, dx, first, count in GROUPS[g]:
                O[dz, dx, first : first + count, cols] = o[done : done + count]
                done += count

    def backward(g):
        product(g)
        run(after.get(g, ()))

    def out_down(r):
        xsa[r] = O[r, 2].astype(BF16)
        c.send(f"d{r}", xsa.at[r], xd.at[r], {1: zp, 3: zm}[r])

    def out_far(r):
        total = O[r, 2]
        if r == 0:
            c.need("d1", "d3")
            total = total + xd[1].astype(F32) + xd[3].astype(F32)
        xsa[r] = total.astype(BF16)
        c.send(f"xa+{r}", xsa.at[r, :, L], xa.at[r // 2, 0], xp, xa.at[r // 2])
        c.send(f"xa-{r}", xsa.at[r, :, R], xa.at[r // 2, 1], xm, xa.at[r // 2])

    def out_pass(r):
        c.need(f"xa+{r}", f"xa-{r}")
        c.send(f"xd+{r}", xa.at[r // 2, 0], xd.at[r, :, L], xp, xd.at[r])
        c.send(f"xd-{r}", xa.at[r // 2, 1], xd.at[r, :, R], xm, xd.at[r])

    def out_near(r, dx, rows=(0, ROWS), halves=(0, 1)):
        k, sign, device = {1: (0, "+", xp), 3: (1, "-", xm)}[dx]
        at, to = slice(*rows), pl.ds(rows[0], rows[1] - rows[0])
        cols = pl.ds(halves[0] * HALF, len(halves) * HALF)
        xsb[r, k, at, cols] = O[r, dx, at, cols].astype(BF16)
        c.send(f"xb{sign}{r}_{rows[0]}_{halves[0]}", xsb.at[r, k, to, cols], xb.at[r, k, to, cols], device)

    def over_x(r, at, cols):
        near = O[r, 0, at, cols] + xb[r, 0, at, cols].astype(F32) + xb[r, 1, at, cols].astype(F32)
        return near + xd[r, at, cols].astype(F32) if r in (0, 2) else near

    def out_sum(r, rows=(0, ROWS), halves=(0, 1)):
        c.need(f"xb+{r}_0_0", f"xb-{r}_0_0")
        if r == 2:
            c.need("xd+2", "xd-2")
        at, to = slice(*rows), pl.ds(rows[0], rows[1] - rows[0])
        cols = pl.ds(halves[0] * HALF, len(halves) * HALF)
        zs[r - 1, at, cols] = over_x(r, at, cols).astype(BF16)
        if r == 2:
            c.send("z2+", zs.at[1, :, L], zt.at[0], zp, zt)
            c.send("z2-", zs.at[1, :, R], zt.at[1], zm, zt)
        else:
            name = f"z{r}_{rows[0]}_{halves[0]}"
            c.send(name, zs.at[r - 1, to, cols], zr.at[r - 1, to, cols], {1: zp, 3: zm}[r])

    def out_sum_far():
        c.need("z2+", "z2-")
        c.send("z2f+", zt.at[0], zr.at[1, :, L], zp, zr.at[1])
        c.send("z2f-", zt.at[1], zr.at[1, :, R], zm, zr.at[1])

    def out_final(first, rows):
        at = slice(first, first + rows)
        total = over_x(0, at, slice(0, WIDTH))
        for k in range(3):
            total += zr[k, at].astype(F32)
        out_ref[at] = total.astype(BF16)

    after = {
        1: ((out_near, 0, 1, (0, EARLY)), (out_near, 0, 3, (0, EARLY))),
        3: ((out_near, 1, 1), (out_near, 3, 3)),
        4: ((out_near, 1, 3), (out_near, 3, 1)),
        5: ((out_far, 2), (out_down, 1), (out_sum, 1, (0, EARLY)), (out_sum, 3, (0, EARLY))),
        6: ((out_down, 3), (out_near, 2, 1), (out_near, 2, 3)),
        7: ((out_far, 0),),
    }

    def run(events):
        for event, *args in events:
            event(*args)

    for n, (q, j) in enumerate(own):
        for k, (src, dst) in enumerate(pieces(q, j)):
            local(src, dst, weight_sems.at[3 * q + k])
    for copy in own_tokens:
        copy.wait()
    forward(0, 0, 1)
    reduce_far(0)
    forward(0, 1, 4)
    reduce_near(0)
    relay_first("", ahead)
    forward(1)
    reduce_far(1)
    relay_first("b", behind)
    relay_1()
    grads(0)
    forward(2)
    reduce_far(2)
    reduce_near(1)
    spread(0)
    forward(3)
    reduce_far(3)
    reduce_near(2)
    relay_2()
    grads(1)
    backward(0)
    reduce_near(3)
    relay_3()
    forward(4)
    spread(1)
    grads(2)
    reduce_far(4)
    relay_4()
    grads(3)
    spread(2)
    backward(1)
    reduce_near(4)
    relays[5]()
    forward(5)
    spread(3)
    for t in range(5, last):
        reduce_far(t)
        if t == 5:
            backward(2)
        grads(t - 1)
        backward(t - 2)
        reduce_near(t)
        if t + 1 in relays:
            relays[t + 1]()
        forward(t + 1)
        spread(t - 1)
    reduce_far(last)
    grads(last - 1)
    out_pass(2)
    backward(last - 2)
    reduce_near(last)
    spread(last - 1)
    grads(last)
    backward(last - 1)
    spread(last)
    out_sum(2)

    def out_last(h):
        out_near(0, 1, (EARLY, ROWS), (h,))
        out_near(0, 3, (EARLY, ROWS), (h,))
        out_sum(1, (EARLY, ROWS), (h,))
        out_sum(3, (EARLY, ROWS), (h,))

    product(last, 0, 2)
    out_last(0)
    out_pass(0)
    product(last, 2, 1)
    out_sum_far()
    product(last, 3, 1)
    out_last(1)
    for copy in locals_:
        copy.wait_send()
    c.finish()
    out_final(0, ROWS // 2)
    out_final(ROWS // 2, ROWS // 2)


def shards(inputs, out_grad, gate_weight, up_weight, down_weight):
    return pl.pallas_call(
        kernel,
        out_shape=pltpu.VMEM((ROWS, WIDTH), BF16),
        in_specs=[pl.BlockSpec(memory_space=pl.ANY)] * 5,
        out_specs=pl.BlockSpec(memory_space=pltpu.VMEM),
        scratch_shapes=[
            pltpu.VMEM((4, 4, ROWS, WIDTH), BF16),
            pltpu.VMEM((4, 4, ROWS, WIDTH), BF16),
            pltpu.VMEM((WIDTH, 8 * Q), BF16),
            pltpu.VMEM((4 * Q, WIDTH), BF16),
            pltpu.VMEM((3, 4, TOP, 3 * Q), F32),
            pltpu.VMEM((4, 4, ROWS, WIDTH), F32),
            pltpu.VMEM((2, ALL, CUT), BF16),
            pltpu.VMEM((2, ALL, 3 * Q), BF16),
            pltpu.VMEM((ALL, 8 * Q), BF16),
            pltpu.VMEM((2, TOP, 3 * Q), BF16),
            pltpu.VMEM((2, 2, TOP, 3 * Q), BF16),
            pltpu.VMEM((4, ROWS, WIDTH), BF16),
            pltpu.VMEM((4, 2, ROWS, WIDTH), BF16),
            pltpu.VMEM((2, 2, ROWS, HALF), BF16),
            pltpu.VMEM((4, 2, ROWS, WIDTH), BF16),
            pltpu.VMEM((4, ROWS, WIDTH), BF16),
            pltpu.VMEM((3, ROWS, WIDTH), BF16),
            pltpu.VMEM((2, ROWS, HALF), BF16),
            pltpu.VMEM((3, ROWS, WIDTH), BF16),
            pltpu.SemaphoreType.DMA((SENDS,)),
            pltpu.SemaphoreType.DMA((RECVS,)),
            pltpu.SemaphoreType.DMA((2,)),
            pltpu.SemaphoreType.DMA((6,)),
            pltpu.SemaphoreType.DMA((12,)),
        ],
        compiler_params=pltpu.CompilerParams(
            collective_id=0, has_side_effects=True, vmem_limit_bytes=66_600_000
        ),
        name="swiglu_back",
    )(inputs, out_grad, gate_weight, up_weight, down_weight)


def solution(mesh):
    return jax.shard_map(
        shards,
        mesh=mesh,
        in_specs=(
            P(("gx", "gz"), "gy"),
            P(("gx", "gz"), "gy"),
            P("gy", ("gx", "gz")),
            P("gy", ("gx", "gz")),
            P(("gx", "gz"), "gy"),
        ),
        out_specs=P(("gx", "gz"), "gy"),
        check_vma=False,
    )
```

```python
import jax
import jax.numpy as jnp
from jax import lax
from jax.experimental import pallas as pl
from jax.experimental.pallas import tpu as pltpu
from jax.sharding import PartitionSpec as P

MESH = pl.DeviceIdType.MESH
F32 = jnp.float32
BF16 = jnp.bfloat16

ROWS = 80
WIDTH = 2048
HALF = WIDTH // 2
OWN = 512
Q = 256
CUT = 3 * Q // 2
PARTS = 2
PART = HALF // PARTS

GROUPS = (
    ((0, 0, 0, 80),),
    ((0, 1, 0, 48), (0, 3, 0, 48)),
    ((1, 0, 0, 48), (3, 0, 0, 48)),
    ((1, 1, 0, 80), (3, 3, 0, 80)),
    ((1, 3, 0, 80), (3, 1, 0, 80)),
    ((2, 2, 0, 80), (1, 2, 0, 80), (2, 1, 0, 48)),
    ((3, 2, 0, 80), (2, 3, 0, 80), (2, 1, 48, 32)),
    ((0, 2, 0, 80), (2, 0, 0, 80)),
    ((1, 0, 48, 32), (3, 0, 48, 32), (0, 1, 48, 32), (0, 3, 48, 32)),
)
EARLY = 48
SIZES = tuple(sum(rows for *_, rows in group) for group in GROUPS)
STARTS = tuple(sum(SIZES[:g]) for g in range(len(SIZES)))
TOP = max(SIZES)
ALL = sum(SIZES)


def contract_last(left, right):
    return lax.dot_general(
        left, right, (((1,), (1,)), ((), ())), preferred_element_type=F32
    )


class Copies:
    def __init__(self, send_sems, recv_sems):
        self.send_sems, self.recv_sems = send_sems, recv_sems
        self.made, self.sent, self.landed = {}, {}, set()
        self.keys, self.user, self.pairs = {}, {}, {}

    def send(self, name, src, dst, device, both=None):
        k = len(self.made) % SENDS
        for old in [old for old, at in self.sent.items() if at == k]:
            self.free(old)
        base = name if both is None else name.replace("+", "").replace("-", "")
        key = base[:2] + str(int(base[2:]) % 3) if base[:2] in OVER_Y else base
        r = self.keys.setdefault(key, len(self.keys))
        assert self.user.get(key, base) == base or self.user[key] in self.landed
        self.user[key] = base
        copy = pltpu.make_async_remote_copy(
            src_ref=src,
            dst_ref=dst,
            send_sem=self.send_sems.at[k],
            recv_sem=self.recv_sems.at[r],
            device_id=device,
            device_id_type=MESH,
        )
        self.made[name] = copy
        self.sent[name] = k
        if both is not None:
            self.pairs[name] = base, (both, both, self.recv_sems.at[r])
        copy.start()

    def need(self, *names):
        for name in names:
            base, pair = self.pairs.get(name, (name, None))
            if base not in self.landed:
                self.landed.add(base)
                if pair is None:
                    self.made[name].wait_recv()
                else:
                    pltpu.make_async_copy(*pair).wait()

    def free(self, *names):
        for name in names:
            if name in self.sent:
                del self.sent[name]
                self.made[name].wait_send()

    def finish(self):
        assert len(self.keys) == RECVS
        self.need(*self.made)
        self.free(*list(self.sent))


OVER_Y = ("ra", "rb", "ga", "gf")
SENDS = 28
RECVS = 86


def kernel(
    x_hbm, g_hbm, wg_hbm, wu_hbm, wd_hbm, out_ref,
    A, B, Wgu, Wd, S, O, ra, rb, H, sa, sb, xsa, xsb, xa, xb, xd, zs, zt, zr,
    send_sems, recv_sems, local_sems, weight_sends, weight_sems,
):
    gx, y, gz = lax.axis_index("gx"), lax.axis_index("gy"), lax.axis_index("gz")
    x = lax.div(gz, 2) * 2 + lax.div(gx, 4)
    z = lax.rem(gx, 4)
    core = lax.rem(gz, 2)

    def device(dx=0, dy=0, dz=0):
        nx, ny, nz = (lax.rem(p + d + 4, 4) for p, d in ((x, dx), (y, dy), (z, dz)))
        return {
            "gx": lax.rem(nx, 2) * 4 + nz,
            "gy": ny,
            "gz": lax.div(nx, 2) * 2 + core,
        }

    partner = {"gx": gx, "gy": y, "gz": gz + 1 - 2 * core}
    xp, xm = device(dx=1), device(dx=-1)
    yp, ym = device(dy=1), device(dy=-1)
    zp, zm = device(dz=1), device(dz=-1)

    barrier = pltpu.get_barrier_semaphore()
    peers = (partner, xp, xm, yp, ym, zp, zm)
    own_tokens = [
        pltpu.make_async_copy(src, ref.at[0, 0], local_sems.at[k])
        for k, (src, ref) in enumerate(((x_hbm, A), (g_hbm, B)))
    ]
    for copy in own_tokens:
        copy.start()
    for peer in peers:
        pl.semaphore_signal(barrier, inc=1, device_id=peer, device_id_type=MESH)
    pl.semaphore_wait(barrier, len(peers))

    c = Copies(send_sems, recv_sems)
    L, R = pl.ds(0, HALF), pl.ds(HALF, HALF)

    near = lax.rem(y + 2, 4)
    mine = 1 - jnp.abs(lax.div(near, 2) - core)
    lead = mine * lax.rem(near, 2)
    locals_ = []

    def local(src, dst, sem):
        copy = pltpu.make_async_copy(src, dst, sem)
        copy.start()
        return copy

    def pieces(q, j):
        wide, narrow = pl.multiple_of(q * 2 * Q, 2 * Q), pl.multiple_of(q * Q, Q)
        part = pl.ds(pl.multiple_of(j * Q, Q), Q)
        return (
            (wg_hbm.at[:, part], Wgu.at[:, pl.ds(wide, Q)]),
            (wu_hbm.at[:, part], Wgu.at[:, pl.ds(wide + Q, Q)]),
            (wd_hbm.at[part], Wd.at[pl.ds(narrow, Q)]),
        )

    own = [(2 * core + j, j) for j in (lead, 1 - lead)]
    for n, (q, j) in enumerate(own):
        for k, (src, dst) in enumerate(pieces(q, j)):
            copy = pltpu.make_async_remote_copy(
                src_ref=src,
                dst_ref=dst,
                send_sem=weight_sends.at[3 * n + k],
                recv_sem=weight_sems.at[3 * q + k],
                device_id=partner,
                device_id_type=MESH,
            )
            copy.start()
            locals_.append(copy)

    def own_over_x(name, hbm, ref, rows):
        c.send(name.replace("@", "+"), hbm.at[rows], ref.at[0, 3, rows], xp)
        c.send(name.replace("@", "-"), hbm.at[rows], ref.at[0, 1, rows], xm)

    def own_over_z(name, hbm, ref, rows):
        c.send(name.replace("@", "+"), hbm.at[rows], ref.at[3, 0, rows], zp)
        c.send(name.replace("@", "-"), hbm.at[rows], ref.at[1, 0, rows], zm)

    ahead, behind = pl.ds(0, EARLY), pl.ds(EARLY, ROWS - EARLY)
    own_over_x("Ax@", x_hbm, A, ahead)
    own_over_z("Bz@", g_hbm, B, ahead)
    own_over_x("Bx@0", g_hbm, B, ahead)
    own_over_z("Az@0", x_hbm, A, ahead)
    own_over_x("Ax@b", x_hbm, A, behind)
    own_over_z("Bz@b", g_hbm, B, behind)

    def need_weights(q):
        for k, (src, dst) in enumerate(pieces(q, 0)):
            pltpu.make_async_copy(src, dst, weight_sems.at[3 * q + k]).wait()

    def a_over_z(dx):
        c.send(f"Az+{dx}", A.at[0, dx], A.at[3, dx], zp)
        c.send(f"Az-{dx}", A.at[0, dx], A.at[1, dx], zm)

    def whole(*names):
        for name in names:
            c.need(name)
            if name + "b" in c.made:
                c.need(name + "b")

    def a_over_z_far(dx):
        whole(f"Az+{dx}", f"Az-{dx}")
        c.send(f"Azf+{dx}", A.at[3, dx, :, L], A.at[2, dx, :, L], zp, A.at[2, dx])
        c.send(f"Azf-{dx}", A.at[1, dx, :, R], A.at[2, dx, :, R], zm, A.at[2, dx])

    def b_over_x(dz):
        c.send(f"Bx+{dz}", B.at[dz, 0], B.at[dz, 3], xp)
        c.send(f"Bx-{dz}", B.at[dz, 0], B.at[dz, 1], xm)

    def b_over_x_far(dz):
        whole(f"Bx+{dz}", f"Bx-{dz}")
        c.send(f"Bxf+{dz}", B.at[dz, 3, :, L], B.at[dz, 2, :, L], xp, B.at[dz, 2])
        c.send(f"Bxf-{dz}", B.at[dz, 1, :, R], B.at[dz, 2, :, R], xm, B.at[dz, 2])

    def relay_first(piece, rows):
        c.need(f"Ax+{piece}", f"Ax-{piece}")
        c.send(f"Az-1{piece}", A.at[0, 1, rows], A.at[1, 1, rows], zm)
        c.send(f"Az+3{piece}", A.at[0, 3, rows], A.at[3, 3, rows], zp)
        c.need(f"Bz+{piece}", f"Bz-{piece}")
        c.send(f"Bx-1{piece}", B.at[1, 0, rows], B.at[1, 1, rows], xm)
        c.send(f"Bx+3{piece}", B.at[3, 0, rows], B.at[3, 3, rows], xp)

    def relay_1():
        c.send("Axf+", A.at[0, 3, :, L], A.at[0, 2, :, L], xp, A.at[0, 2])
        c.send("Axf-", A.at[0, 1, :, R], A.at[0, 2, :, R], xm, A.at[0, 2])
        c.send("Bzf+", B.at[3, 0, :, L], B.at[2, 0, :, L], zp, B.at[2, 0])
        c.send("Bzf-", B.at[1, 0, :, R], B.at[2, 0, :, R], zm, B.at[2, 0])
        c.send("Az+1", A.at[0, 1], A.at[3, 1], zp)
        c.send("Az-3", A.at[0, 3], A.at[1, 3], zm)
        c.send("Bx+1", B.at[1, 0], B.at[1, 3], xp)
        c.send("Bx-3", B.at[3, 0], B.at[3, 1], xm)

    def relay_2():
        c.need("Bzf+", "Bzf-")
        b_over_x(2)
        c.need("Axf+", "Axf-")
        a_over_z(2)

    def relay_3():
        b_over_x_far(1)
        a_over_z_far(1)

    def relay_4():
        a_over_z_far(2)
        b_over_x_far(2)
        a_over_z_far(3)
        b_over_x_far(3)
        own_over_z("Az@0b", x_hbm, A, behind)

    def relay_5():
        own_over_x("Bx@0b", g_hbm, B, behind)

    def relay_6():
        a_over_z_far(0)
        b_over_x_far(0)

    relays = {5: relay_5, 6: relay_6}

    def need_tokens(g):
        for dz, dx, first, _ in GROUPS[g]:
            late = first >= EARLY
            if dz == 0:
                c.need(*{0: (), 1: ("Ax-", "Bx-0"), 2: ("Axf+", "Axf-", "Bxf+0", "Bxf-0"), 3: ("Ax+", "Bx+0")}[dx])
                if late:
                    c.need(*{0: (), 1: ("Ax-b", "Bx-0b"), 2: (), 3: ("Ax+b", "Bx+0b")}[dx])
                continue
            need = c.need if dx == 0 else whole
            need(*{1: (f"Az-{dx}",), 2: (f"Azf+{dx}", f"Azf-{dx}"), 3: (f"Az+{dx}",)}[dz])
            if dx == 0:
                c.need(*{1: ("Bz-",), 2: ("Bzf+", "Bzf-"), 3: ("Bz+",)}[dz])
                if late:
                    c.need(*{1: ("Az-0b", "Bz-b"), 2: (), 3: ("Az+0b", "Bz+b")}[dz])
            else:
                whole(*{1: (f"Bx-{dz}",), 2: (f"Bxf+{dz}", f"Bxf-{dz}"), 3: (f"Bx+{dz}",)}[dx])

    def rows_of(ref, g):
        parts = [ref[dz, dx, first : first + rows] for dz, dx, first, rows in GROUPS[g]]
        return parts[0] if len(parts) == 1 else jnp.concatenate(parts, axis=0)

    def quarter(k):
        return lax.rem(y + k, 4)

    def forward(g, start=0, stop=4):
        m = SIZES[g]
        need_tokens(g)

        @pl.loop(start, stop)
        def _(k):
            q = lax.rem(y + 2 + k, 4)
            if g == 0:
                need_weights(q)
            w = Wgu[:, pl.ds(pl.multiple_of(q * 2 * Q, 2 * Q), 2 * Q)]
            S[g % 3, k, 0:m, 0 : 2 * Q] = jnp.dot(rows_of(A, g), w, preferred_element_type=F32)
            d = Wd[pl.ds(pl.multiple_of(q * Q, Q), Q), :]
            S[g % 3, k, 0:m, 2 * Q : 3 * Q] = contract_last(rows_of(B, g), d)

    def reduce_far(g):
        s, v, m = g % 2, g % 3, SIZES[g]
        at = pl.ds(STARTS[g], m)
        if g >= 2:
            c.free(f"ra+{g - 2}", f"ra-{g - 2}")
        sa[s, 0:m] = S[v, 0, 0:m].astype(BF16)
        c.send(f"ra+{g}", sa.at[s, pl.ds(0, m), pl.ds(0, CUT)], ra.at[0, at], yp, ra.at[:, at])
        c.send(f"ra-{g}", sa.at[s, pl.ds(0, m), pl.ds(CUT, CUT)], ra.at[1, at], ym, ra.at[:, at])

    def reduce_near(g):
        s, v, m = g % 2, g % 3, SIZES[g]
        at, rows = slice(STARTS[g], STARTS[g] + m), pl.ds(STARTS[g], m)
        if g >= 2:
            c.free(f"rb+{g - 2}", f"rb-{g - 2}")
        c.need(f"ra+{g}", f"ra-{g}")
        sb[s, 0, 0:m, 0:CUT] = (S[v, 3, 0:m, 0:CUT] + ra[0, at].astype(F32)).astype(BF16)
        sb[s, 0, 0:m, CUT:] = S[v, 3, 0:m, CUT:].astype(BF16)
        c.send(f"rb+{g}", sb.at[s, 0, pl.ds(0, m)], rb.at[0, rows], yp, rb.at[:, rows])
        sb[s, 1, 0:m, 0:CUT] = S[v, 1, 0:m, 0:CUT].astype(BF16)
        sb[s, 1, 0:m, CUT:] = (S[v, 1, 0:m, CUT:] + ra[1, at].astype(F32)).astype(BF16)
        c.send(f"rb-{g}", sb.at[s, 1, pl.ds(0, m)], rb.at[1, rows], ym, rb.at[:, rows])

    last = len(GROUPS) - 1

    def grads(g):
        v, m = g % 3, SIZES[g]
        rows = pl.ds(STARTS[g], m)
        c.need(f"rb+{g}", f"rb-{g}")

        def total(at):
            cols = pl.ds(at, Q)
            return S[v, 2, 0:m, cols] + rb[0, rows, cols].astype(F32) + rb[1, rows, cols].astype(F32)

        gate, upper, hidden_grad = total(0), total(Q), total(2 * Q)
        logistic = 1.0 / (1.0 + jnp.exp(-gate))
        scaled = hidden_grad * logistic
        at = pl.multiple_of(y * (2 * Q), 2 * Q)
        H[rows, pl.ds(at, Q)] = (scaled * upper * (1.0 + gate * (1.0 - logistic))).astype(BF16)
        H[rows, pl.ds(at + Q, Q)] = (scaled * gate).astype(BF16)
        own = H.at[rows, pl.ds(at, 2 * Q)]
        c.send(f"ga+{g}", own, own, yp, H.at[rows, pl.ds(0, 4 * Q)])
        c.send(f"ga-{g}", own, own, ym, H.at[rows, pl.ds(0, 4 * Q)])

    def spread(g):
        rows = pl.ds(STARTS[g], SIZES[g])
        c.need(f"ga+{g}", f"ga-{g}")
        at = pl.multiple_of(quarter(3) * (2 * Q), 2 * Q)
        part = H.at[rows, pl.ds(at, Q)]
        c.send(f"gf+{g}", part, part, yp, H.at[rows, pl.ds(0, 2 * Q)])
        at = pl.multiple_of(quarter(1) * (2 * Q), 2 * Q)
        part = H.at[rows, pl.ds(at + Q, Q)]
        c.send(f"gf-{g}", part, part, ym, H.at[rows, pl.ds(0, 2 * Q)])

    def product(g, start=0, steps=4):
        rows = slice(STARTS[g], STARTS[g] + SIZES[g])
        c.need(f"gf+{g}", f"gf-{g}")

        @pl.loop(start, start + steps)
        def _(n):
            cols = pl.ds(pl.multiple_of(n * 512, 512), 512)
            o = contract_last(H[rows], Wgu[cols, :])
            done = 0
            for dz, dx, first, count in GROUPS[g]:
                O[dz, dx, first : first + count, cols] = o[done : done + count]
                done += count

    def backward(g, between=None):
        if between is None:
            product(g)
        else:
            product(g, 0, 2)
            reduce_near(between)
            product(g, 2, 2)
        run(after.get(g, ()))

    def out_down(r):
        xsa[r] = O[r, 2].astype(BF16)
        c.send(f"d{r}", xsa.at[r], xd.at[r], {1: zp, 3: zm}[r])

    def out_far(r):
        total = O[r, 2]
        if r == 0:
            c.need("d1", "d3")
            total = total + xd[1].astype(F32) + xd[3].astype(F32)
        xsa[r] = total.astype(BF16)
        for p in range(PARTS):
            here, there = pl.ds(p * PART, PART), pl.ds(HALF + p * PART, PART)
            both = xa.at[r // 2, :, :, here]
            c.send(f"xa+{r}_{p}", xsa.at[r, :, here], xa.at[r // 2, 0, :, here], xp, both)
            c.send(f"xa-{r}_{p}", xsa.at[r, :, there], xa.at[r // 2, 1, :, here], xm, both)

    def out_pass(r, p):
        here, there = pl.ds(p * PART, PART), pl.ds(HALF + p * PART, PART)
        both = xd.at[r, :, pl.ds(0, 2 * PART)]
        c.need(f"xa+{r}_{p}", f"xa-{r}_{p}")
        c.send(f"xd+{r}_{p}", xa.at[r // 2, 0, :, here], xd.at[r, :, here], xp, both)
        c.send(f"xd-{r}_{p}", xa.at[r // 2, 1, :, here], xd.at[r, :, there], xm, both)

    def out_near(r, dx, rows=(0, ROWS), halves=(0, 1)):
        k, sign, device = {1: (0, "+", xp), 3: (1, "-", xm)}[dx]
        at, to = slice(*rows), pl.ds(rows[0], rows[1] - rows[0])
        cols = pl.ds(halves[0] * HALF, len(halves) * HALF)
        xsb[r, k, at, cols] = O[r, dx, at, cols].astype(BF16)
        c.send(f"xb{sign}{r}_{rows[0]}_{halves[0]}", xsb.at[r, k, to, cols], xb.at[r, k, to, cols], device)

    def over_x(r, at, cols):
        near = O[r, 0, at, cols] + xb[r, 0, at, cols].astype(F32) + xb[r, 1, at, cols].astype(F32)
        return near + xd[r, at, cols].astype(F32) if r in (0, 2) else near

    def out_sum(r, rows=(0, ROWS), halves=(0, 1)):
        c.need(f"xb+{r}_0_0", f"xb-{r}_0_0")
        if r == 2:
            c.need(*(f"xd+2_{p}" for p in range(PARTS)))
        at, to = slice(*rows), pl.ds(rows[0], rows[1] - rows[0])
        cols = pl.ds(halves[0] * HALF, len(halves) * HALF)
        zs[r - 1, at, cols] = over_x(r, at, cols).astype(BF16)
        if r == 2:
            for p in range(PARTS):
                here, there = pl.ds(p * PART, PART), pl.ds(HALF + p * PART, PART)
                both = zt.at[:, :, here]
                c.send(f"z2+{p}", zs.at[1, :, here], zt.at[0, :, here], zp, both)
                c.send(f"z2-{p}", zs.at[1, :, there], zt.at[1, :, here], zm, both)
        else:
            name = f"z{r}_{rows[0]}_{halves[0]}"
            c.send(name, zs.at[r - 1, to, cols], zr.at[r - 1, to, cols], {1: zp, 3: zm}[r])

    def out_sum_far(p):
        here, there = pl.ds(p * PART, PART), pl.ds(HALF + p * PART, PART)
        both = zr.at[1, :, pl.ds(0, 2 * PART)]
        c.need(f"z2+{p}", f"z2-{p}")
        c.send(f"z2f+{p}", zt.at[0, :, here], zr.at[1, :, here], zp, both)
        c.send(f"z2f-{p}", zt.at[1, :, here], zr.at[1, :, there], zm, both)

    def out_final(first, rows):
        at = slice(first, first + rows)
        total = over_x(0, at, slice(0, WIDTH))
        for k in range(3):
            total += zr[k, at].astype(F32)
        out_ref[at] = total.astype(BF16)

    after = {
        1: ((out_near, 0, 1, (0, EARLY)), (out_near, 0, 3, (0, EARLY))),
        3: ((out_near, 1, 1), (out_near, 3, 3)),
        4: ((out_near, 1, 3), (out_near, 3, 1)),
        5: ((out_far, 2), (out_down, 1), (out_sum, 1, (0, EARLY)), (out_sum, 3, (0, EARLY))),
        6: ((out_down, 3), (out_near, 2, 1), (out_near, 2, 3)),
        7: ((out_far, 0),),
    }

    def run(events):
        for event, *args in events:
            event(*args)

    for n, (q, j) in enumerate(own):
        for k, (src, dst) in enumerate(pieces(q, j)):
            local(src, dst, weight_sems.at[3 * q + k])
    for copy in own_tokens:
        copy.wait()
    forward(0, 0, 1)
    reduce_far(0)
    forward(0, 1, 4)
    reduce_near(0)
    relay_first("", ahead)
    forward(1)
    reduce_far(1)
    relay_first("b", behind)
    relay_1()
    grads(0)
    forward(2)
    reduce_far(2)
    reduce_near(1)
    spread(0)
    forward(3)
    reduce_far(3)
    reduce_near(2)
    relay_2()
    grads(1)
    backward(0)
    reduce_near(3)
    relay_3()
    forward(4)
    spread(1)
    grads(2)
    reduce_far(4)
    relay_4()
    grads(3)
    spread(2)
    backward(1)
    reduce_near(4)
    relays[5]()
    forward(5)
    spread(3)
    for t in range(5, last):
        reduce_far(t)
        if t == 5:
            backward(2)
        grads(t - 1)
        backward(t - 2, t)
        if t + 1 in relays:
            relays[t + 1]()
        forward(t + 1)
        spread(t - 1)
    reduce_far(last)
    grads(last - 1)
    for p in range(PARTS):
        out_pass(2, p)
    backward(last - 2, last)
    spread(last - 1)
    grads(last)
    backward(last - 1)
    spread(last)
    out_sum(2)

    def out_last(h):
        out_near(0, 1, (EARLY, ROWS), (h,))
        out_near(0, 3, (EARLY, ROWS), (h,))
        out_sum(1, (EARLY, ROWS), (h,))
        out_sum(3, (EARLY, ROWS), (h,))

    product(last, 0, 1)
    out_pass(0, 0)
    out_sum_far(0)
    product(last, 1, 1)
    out_last(0)
    out_pass(0, 1)
    out_sum_far(1)
    product(last, 2, 2)
    out_last(1)
    for copy in locals_:
        copy.wait_send()
    c.finish()
    out_final(0, ROWS // 2)
    out_final(ROWS // 2, ROWS // 2)


def shards(inputs, out_grad, gate_weight, up_weight, down_weight):
    return pl.pallas_call(
        kernel,
        out_shape=pltpu.VMEM((ROWS, WIDTH), BF16),
        in_specs=[pl.BlockSpec(memory_space=pl.ANY)] * 5,
        out_specs=pl.BlockSpec(memory_space=pltpu.VMEM),
        scratch_shapes=[
            pltpu.VMEM((4, 4, ROWS, WIDTH), BF16),
            pltpu.VMEM((4, 4, ROWS, WIDTH), BF16),
            pltpu.VMEM((WIDTH, 8 * Q), BF16),
            pltpu.VMEM((4 * Q, WIDTH), BF16),
            pltpu.VMEM((3, 4, TOP, 3 * Q), F32),
            pltpu.VMEM((4, 4, ROWS, WIDTH), F32),
            pltpu.VMEM((2, ALL, CUT), BF16),
            pltpu.VMEM((2, ALL, 3 * Q), BF16),
            pltpu.VMEM((ALL, 8 * Q), BF16),
            pltpu.VMEM((2, TOP, 3 * Q), BF16),
            pltpu.VMEM((2, 2, TOP, 3 * Q), BF16),
            pltpu.VMEM((4, ROWS, WIDTH), BF16),
            pltpu.VMEM((4, 2, ROWS, WIDTH), BF16),
            pltpu.VMEM((2, 2, ROWS, HALF), BF16),
            pltpu.VMEM((4, 2, ROWS, WIDTH), BF16),
            pltpu.VMEM((4, ROWS, WIDTH), BF16),
            pltpu.VMEM((3, ROWS, WIDTH), BF16),
            pltpu.VMEM((2, ROWS, HALF), BF16),
            pltpu.VMEM((3, ROWS, WIDTH), BF16),
            pltpu.SemaphoreType.DMA((SENDS,)),
            pltpu.SemaphoreType.DMA((RECVS,)),
            pltpu.SemaphoreType.DMA((2,)),
            pltpu.SemaphoreType.DMA((6,)),
            pltpu.SemaphoreType.DMA((12,)),
        ],
        compiler_params=pltpu.CompilerParams(
            collective_id=0, has_side_effects=True, vmem_limit_bytes=66_600_000
        ),
        name="swiglu_back",
    )(inputs, out_grad, gate_weight, up_weight, down_weight)


def solution(mesh):
    return jax.shard_map(
        shards,
        mesh=mesh,
        in_specs=(
            P(("gx", "gz"), "gy"),
            P(("gx", "gz"), "gy"),
            P("gy", ("gx", "gz")),
            P("gy", ("gx", "gz")),
            P(("gx", "gz"), "gy"),
        ),
        out_specs=P(("gx", "gz"), "gy"),
        check_vma=False,
    )
```

```python
import jax
import jax.numpy as jnp
from jax import lax
from jax.experimental import pallas as pl
from jax.experimental.pallas import tpu as pltpu
from jax.sharding import PartitionSpec as P

MESH = pl.DeviceIdType.MESH
F32 = jnp.float32
BF16 = jnp.bfloat16

ROWS = 80
WIDTH = 2048
HALF = WIDTH // 2
OWN = 512
Q = 256
CUT = 3 * Q // 2
PARTS = 2
PART = HALF // PARTS

GROUPS = (
    ((0, 0, 0, 80),),
    ((0, 1, 0, 48), (0, 3, 0, 48)),
    ((1, 0, 0, 48), (3, 0, 0, 48)),
    ((1, 1, 0, 80), (3, 3, 0, 80)),
    ((1, 3, 0, 80), (3, 1, 0, 80)),
    ((2, 2, 0, 80), (1, 2, 0, 80), (2, 1, 0, 48)),
    ((3, 2, 0, 80), (2, 3, 0, 80), (2, 1, 48, 32)),
    ((0, 2, 0, 80), (2, 0, 0, 80)),
    ((1, 0, 48, 32), (3, 0, 48, 32), (0, 1, 48, 32), (0, 3, 48, 32)),
)
EARLY = 48
SIZES = tuple(sum(rows for *_, rows in group) for group in GROUPS)
STARTS = tuple(sum(SIZES[:g]) for g in range(len(SIZES)))
TOP = max(SIZES)
ALL = sum(SIZES)


def contract_last(left, right):
    return lax.dot_general(
        left, right, (((1,), (1,)), ((), ())), preferred_element_type=F32
    )


class Copies:
    def __init__(self, send_sems, recv_sems):
        self.send_sems, self.recv_sems = send_sems, recv_sems
        self.made, self.sent, self.landed = {}, {}, set()
        self.keys, self.user, self.pairs = {}, {}, {}

    def send(self, name, src, dst, device, both=None):
        k = len(self.made) % SENDS
        for old in [old for old, at in self.sent.items() if at == k]:
            self.free(old)
        base = name if both is None else name.replace("+", "").replace("-", "")
        key = base[:2] + str(int(base[2:]) % 3) if base[:2] in OVER_Y else base
        r = self.keys.setdefault(key, len(self.keys))
        assert self.user.get(key, base) == base or self.user[key] in self.landed
        self.user[key] = base
        copy = pltpu.make_async_remote_copy(
            src_ref=src,
            dst_ref=dst,
            send_sem=self.send_sems.at[k],
            recv_sem=self.recv_sems.at[r],
            device_id=device,
            device_id_type=MESH,
        )
        self.made[name] = copy
        self.sent[name] = k
        if both is not None:
            self.pairs[name] = base, (both, both, self.recv_sems.at[r])
        copy.start()

    def need(self, *names):
        for name in names:
            base, pair = self.pairs.get(name, (name, None))
            if base not in self.landed:
                self.landed.add(base)
                if pair is None:
                    self.made[name].wait_recv()
                else:
                    pltpu.make_async_copy(*pair).wait()

    def free(self, *names):
        for name in names:
            if name in self.sent:
                del self.sent[name]
                self.made[name].wait_send()

    def finish(self):
        assert len(self.keys) == RECVS
        self.need(*self.made)
        self.free(*list(self.sent))


OVER_Y = ("ra", "rb", "ga", "gf")
SENDS = 24
RECVS = 86


def kernel(
    x_hbm, g_hbm, wg_hbm, wu_hbm, wd_hbm, out_ref,
    A, B, Wgu, Wd, S, O, ra, rb, H, sa, sb, xsa, xsb, xa, xb, xd, zs, zt, zr,
    send_sems, recv_sems, local_sems, weight_sends, weight_sems,
):
    gx, y, gz = lax.axis_index("gx"), lax.axis_index("gy"), lax.axis_index("gz")
    x = lax.div(gz, 2) * 2 + lax.div(gx, 4)
    z = lax.rem(gx, 4)
    core = lax.rem(gz, 2)

    def device(dx=0, dy=0, dz=0):
        nx, ny, nz = (lax.rem(p + d + 4, 4) for p, d in ((x, dx), (y, dy), (z, dz)))
        return {
            "gx": lax.rem(nx, 2) * 4 + nz,
            "gy": ny,
            "gz": lax.div(nx, 2) * 2 + core,
        }

    partner = {"gx": gx, "gy": y, "gz": gz + 1 - 2 * core}
    xp, xm = device(dx=1), device(dx=-1)
    yp, ym = device(dy=1), device(dy=-1)
    zp, zm = device(dz=1), device(dz=-1)

    barrier = pltpu.get_barrier_semaphore()
    peers = (partner, xp, xm, yp, ym, zp, zm)
    own_tokens = [
        pltpu.make_async_copy(src, ref.at[0, 0], local_sems.at[k])
        for k, (src, ref) in enumerate(((x_hbm, A), (g_hbm, B)))
    ]
    for copy in own_tokens:
        copy.start()
    for peer in peers:
        pl.semaphore_signal(barrier, inc=1, device_id=peer, device_id_type=MESH)
    pl.semaphore_wait(barrier, len(peers))

    c = Copies(send_sems, recv_sems)
    L, R = pl.ds(0, HALF), pl.ds(HALF, HALF)

    near = lax.rem(y + 2, 4)
    mine = 1 - jnp.abs(lax.div(near, 2) - core)
    lead = mine * lax.rem(near, 2)
    locals_ = []

    def local(src, dst, sem):
        copy = pltpu.make_async_copy(src, dst, sem)
        copy.start()
        return copy

    def pieces(q, j):
        wide, narrow = pl.multiple_of(q * 2 * Q, 2 * Q), pl.multiple_of(q * Q, Q)
        part = pl.ds(pl.multiple_of(j * Q, Q), Q)
        return (
            (wg_hbm.at[:, part], Wgu.at[:, pl.ds(wide, Q)]),
            (wu_hbm.at[:, part], Wgu.at[:, pl.ds(wide + Q, Q)]),
            (wd_hbm.at[part], Wd.at[pl.ds(narrow, Q)]),
        )

    own = [(2 * core + j, j) for j in (lead, 1 - lead)]
    for n, (q, j) in enumerate(own):
        for k, (src, dst) in enumerate(pieces(q, j)):
            copy = pltpu.make_async_remote_copy(
                src_ref=src,
                dst_ref=dst,
                send_sem=weight_sends.at[3 * n + k],
                recv_sem=weight_sems.at[2 * q + k // 2],
                device_id=partner,
                device_id_type=MESH,
            )
            copy.start()
            locals_.append(copy)

    def own_over_x(name, hbm, ref, rows):
        c.send(name.replace("@", "+"), hbm.at[rows], ref.at[0, 3, rows], xp)
        c.send(name.replace("@", "-"), hbm.at[rows], ref.at[0, 1, rows], xm)

    def own_over_z(name, hbm, ref, rows):
        c.send(name.replace("@", "+"), hbm.at[rows], ref.at[3, 0, rows], zp)
        c.send(name.replace("@", "-"), hbm.at[rows], ref.at[1, 0, rows], zm)

    ahead, behind = pl.ds(0, EARLY), pl.ds(EARLY, ROWS - EARLY)
    own_over_x("Ax@", x_hbm, A, ahead)
    own_over_z("Bz@", g_hbm, B, ahead)
    own_over_x("Bx@0", g_hbm, B, ahead)
    own_over_z("Az@0", x_hbm, A, ahead)
    own_over_x("Ax@b", x_hbm, A, behind)
    own_over_z("Bz@b", g_hbm, B, behind)

    def need_weights(q):
        wide = Wgu.at[:, pl.ds(pl.multiple_of(q * 2 * Q, 2 * Q), 2 * Q)]
        narrow = Wd.at[pl.ds(pl.multiple_of(q * Q, Q), Q)]
        for k, ref in enumerate((wide, narrow)):
            pltpu.make_async_copy(ref, ref, weight_sems.at[2 * q + k]).wait()

    def a_over_z(dx):
        c.send(f"Az+{dx}", A.at[0, dx], A.at[3, dx], zp)
        c.send(f"Az-{dx}", A.at[0, dx], A.at[1, dx], zm)

    def whole(*names):
        for name in names:
            c.need(name)
            if name + "b" in c.made:
                c.need(name + "b")

    def a_over_z_far(dx):
        whole(f"Az+{dx}", f"Az-{dx}")
        c.send(f"Azf+{dx}", A.at[3, dx, :, L], A.at[2, dx, :, L], zp, A.at[2, dx])
        c.send(f"Azf-{dx}", A.at[1, dx, :, R], A.at[2, dx, :, R], zm, A.at[2, dx])

    def b_over_x(dz):
        c.send(f"Bx+{dz}", B.at[dz, 0], B.at[dz, 3], xp)
        c.send(f"Bx-{dz}", B.at[dz, 0], B.at[dz, 1], xm)

    def b_over_x_far(dz):
        whole(f"Bx+{dz}", f"Bx-{dz}")
        c.send(f"Bxf+{dz}", B.at[dz, 3, :, L], B.at[dz, 2, :, L], xp, B.at[dz, 2])
        c.send(f"Bxf-{dz}", B.at[dz, 1, :, R], B.at[dz, 2, :, R], xm, B.at[dz, 2])

    def relay_first(piece, rows):
        c.need(f"Ax+{piece}", f"Ax-{piece}")
        c.send(f"Az-1{piece}", A.at[0, 1, rows], A.at[1, 1, rows], zm)
        c.send(f"Az+3{piece}", A.at[0, 3, rows], A.at[3, 3, rows], zp)
        c.need(f"Bz+{piece}", f"Bz-{piece}")
        c.send(f"Bx-1{piece}", B.at[1, 0, rows], B.at[1, 1, rows], xm)
        c.send(f"Bx+3{piece}", B.at[3, 0, rows], B.at[3, 3, rows], xp)

    def relay_1():
        c.send("Axf+", A.at[0, 3, :, L], A.at[0, 2, :, L], xp, A.at[0, 2])
        c.send("Axf-", A.at[0, 1, :, R], A.at[0, 2, :, R], xm, A.at[0, 2])
        c.send("Bzf+", B.at[3, 0, :, L], B.at[2, 0, :, L], zp, B.at[2, 0])
        c.send("Bzf-", B.at[1, 0, :, R], B.at[2, 0, :, R], zm, B.at[2, 0])
        c.send("Az+1", A.at[0, 1], A.at[3, 1], zp)
        c.send("Az-3", A.at[0, 3], A.at[1, 3], zm)
        c.send("Bx+1", B.at[1, 0], B.at[1, 3], xp)
        c.send("Bx-3", B.at[3, 0], B.at[3, 1], xm)

    def relay_2():
        c.need("Bzf+", "Bzf-")
        b_over_x(2)
        c.need("Axf+", "Axf-")
        a_over_z(2)

    def relay_3():
        b_over_x_far(1)
        a_over_z_far(1)

    def relay_4():
        a_over_z_far(2)
        b_over_x_far(2)
        a_over_z_far(3)
        b_over_x_far(3)
        own_over_z("Az@0b", x_hbm, A, behind)

    def relay_5():
        own_over_x("Bx@0b", g_hbm, B, behind)

    def relay_6():
        a_over_z_far(0)
        b_over_x_far(0)

    relays = {5: relay_5, 6: relay_6}

    def need_tokens(g):
        for dz, dx, first, _ in GROUPS[g]:
            late = first >= EARLY
            if dz == 0:
                c.need(*{0: (), 1: ("Ax-", "Bx-0"), 2: ("Axf+", "Axf-", "Bxf+0", "Bxf-0"), 3: ("Ax+", "Bx+0")}[dx])
                if late:
                    c.need(*{0: (), 1: ("Ax-b", "Bx-0b"), 2: (), 3: ("Ax+b", "Bx+0b")}[dx])
                continue
            need = c.need if dx == 0 else whole
            need(*{1: (f"Az-{dx}",), 2: (f"Azf+{dx}", f"Azf-{dx}"), 3: (f"Az+{dx}",)}[dz])
            if dx == 0:
                c.need(*{1: ("Bz-",), 2: ("Bzf+", "Bzf-"), 3: ("Bz+",)}[dz])
                if late:
                    c.need(*{1: ("Az-0b", "Bz-b"), 2: (), 3: ("Az+0b", "Bz+b")}[dz])
            else:
                whole(*{1: (f"Bx-{dz}",), 2: (f"Bxf+{dz}", f"Bxf-{dz}"), 3: (f"Bx+{dz}",)}[dx])

    def rows_of(ref, g):
        parts = [ref[dz, dx, first : first + rows] for dz, dx, first, rows in GROUPS[g]]
        return parts[0] if len(parts) == 1 else jnp.concatenate(parts, axis=0)

    def quarter(k):
        return lax.rem(y + k, 4)

    def forward(g, start=0, stop=4):
        m = SIZES[g]
        need_tokens(g)

        @pl.loop(start, stop)
        def _(k):
            q = lax.rem(y + 2 + k, 4)
            if g == 0:
                need_weights(q)
            w = Wgu[:, pl.ds(pl.multiple_of(q * 2 * Q, 2 * Q), 2 * Q)]
            S[g % 3, k, 0:m, 0 : 2 * Q] = jnp.dot(rows_of(A, g), w, preferred_element_type=F32)
            d = Wd[pl.ds(pl.multiple_of(q * Q, Q), Q), :]
            S[g % 3, k, 0:m, 2 * Q : 3 * Q] = contract_last(rows_of(B, g), d)

    def reduce_far(g):
        s, v, m = g % 2, g % 3, SIZES[g]
        at = pl.ds(STARTS[g], m)
        if g >= 2:
            c.free(f"ra+{g - 2}", f"ra-{g - 2}")
        sa[s, 0:m] = S[v, 0, 0:m].astype(BF16)
        c.send(f"ra+{g}", sa.at[s, pl.ds(0, m), pl.ds(0, CUT)], ra.at[0, at], yp, ra.at[:, at])
        c.send(f"ra-{g}", sa.at[s, pl.ds(0, m), pl.ds(CUT, CUT)], ra.at[1, at], ym, ra.at[:, at])

    def reduce_near(g):
        s, v, m = g % 2, g % 3, SIZES[g]
        at, rows = slice(STARTS[g], STARTS[g] + m), pl.ds(STARTS[g], m)
        if g >= 2:
            c.free(f"rb+{g - 2}", f"rb-{g - 2}")
        c.need(f"ra+{g}", f"ra-{g}")
        sb[s, 0, 0:m, 0:CUT] = (S[v, 3, 0:m, 0:CUT] + ra[0, at].astype(F32)).astype(BF16)
        sb[s, 0, 0:m, CUT:] = S[v, 3, 0:m, CUT:].astype(BF16)
        c.send(f"rb+{g}", sb.at[s, 0, pl.ds(0, m)], rb.at[0, rows], yp, rb.at[:, rows])
        sb[s, 1, 0:m, 0:CUT] = S[v, 1, 0:m, 0:CUT].astype(BF16)
        sb[s, 1, 0:m, CUT:] = (S[v, 1, 0:m, CUT:] + ra[1, at].astype(F32)).astype(BF16)
        c.send(f"rb-{g}", sb.at[s, 1, pl.ds(0, m)], rb.at[1, rows], ym, rb.at[:, rows])

    last = len(GROUPS) - 1

    def grads(g):
        v, m = g % 3, SIZES[g]
        rows = pl.ds(STARTS[g], m)
        c.need(f"rb+{g}", f"rb-{g}")

        def total(at):
            cols = pl.ds(at, Q)
            return S[v, 2, 0:m, cols] + rb[0, rows, cols].astype(F32) + rb[1, rows, cols].astype(F32)

        gate, upper, hidden_grad = total(0), total(Q), total(2 * Q)
        logistic = 1.0 / (1.0 + jnp.exp(-gate))
        scaled = hidden_grad * logistic
        at = pl.multiple_of(y * (2 * Q), 2 * Q)
        H[rows, pl.ds(at, Q)] = (scaled * upper * (1.0 + gate * (1.0 - logistic))).astype(BF16)
        H[rows, pl.ds(at + Q, Q)] = (scaled * gate).astype(BF16)
        own = H.at[rows, pl.ds(at, 2 * Q)]
        c.send(f"ga+{g}", own, own, yp, H.at[rows, pl.ds(0, 4 * Q)])
        c.send(f"ga-{g}", own, own, ym, H.at[rows, pl.ds(0, 4 * Q)])

    def spread(g):
        rows = pl.ds(STARTS[g], SIZES[g])
        c.need(f"ga+{g}", f"ga-{g}")
        at = pl.multiple_of(quarter(3) * (2 * Q), 2 * Q)
        part = H.at[rows, pl.ds(at, Q)]
        c.send(f"gf+{g}", part, part, yp, H.at[rows, pl.ds(0, 2 * Q)])
        at = pl.multiple_of(quarter(1) * (2 * Q), 2 * Q)
        part = H.at[rows, pl.ds(at + Q, Q)]
        c.send(f"gf-{g}", part, part, ym, H.at[rows, pl.ds(0, 2 * Q)])

    def product(g, start=0, steps=4):
        rows = slice(STARTS[g], STARTS[g] + SIZES[g])
        c.need(f"gf+{g}", f"gf-{g}")

        @pl.loop(start, start + steps)
        def _(n):
            cols = pl.ds(pl.multiple_of(n * 512, 512), 512)
            o = contract_last(H[rows], Wgu[cols, :])
            done = 0
            for dz, dx, first, count in GROUPS[g]:
                O[dz, dx, first : first + count, cols] = o[done : done + count]
                done += count

    def backward(g, between=None):
        if between is None:
            product(g)
        else:
            product(g, 0, 2)
            reduce_near(between)
            product(g, 2, 2)
        run(after.get(g, ()))

    def out_down(r):
        xsa[r] = O[r, 2].astype(BF16)
        c.send(f"d{r}", xsa.at[r], xd.at[r], {1: zp, 3: zm}[r])

    def out_far(r):
        total = O[r, 2]
        if r == 0:
            c.need("d1", "d3")
            total = total + xd[1].astype(F32) + xd[3].astype(F32)
        xsa[r] = total.astype(BF16)
        for p in range(PARTS):
            here, there = pl.ds(p * PART, PART), pl.ds(HALF + p * PART, PART)
            both = xa.at[r // 2, :, :, here]
            c.send(f"xa+{r}_{p}", xsa.at[r, :, here], xa.at[r // 2, 0, :, here], xp, both)
            c.send(f"xa-{r}_{p}", xsa.at[r, :, there], xa.at[r // 2, 1, :, here], xm, both)

    def out_pass(r, p):
        here, there = pl.ds(p * PART, PART), pl.ds(HALF + p * PART, PART)
        both = xd.at[r, :, pl.ds(0, 2 * PART)]
        c.need(f"xa+{r}_{p}", f"xa-{r}_{p}")
        c.send(f"xd+{r}_{p}", xa.at[r // 2, 0, :, here], xd.at[r, :, here], xp, both)
        c.send(f"xd-{r}_{p}", xa.at[r // 2, 1, :, here], xd.at[r, :, there], xm, both)

    def out_near(r, dx, rows=(0, ROWS), halves=(0, 1)):
        k, sign, device = {1: (0, "+", xp), 3: (1, "-", xm)}[dx]
        at, to = slice(*rows), pl.ds(rows[0], rows[1] - rows[0])
        cols = pl.ds(halves[0] * HALF, len(halves) * HALF)
        xsb[r, k, at, cols] = O[r, dx, at, cols].astype(BF16)
        c.send(f"xb{sign}{r}_{rows[0]}_{halves[0]}", xsb.at[r, k, to, cols], xb.at[r, k, to, cols], device)

    def over_x(r, at, cols):
        near = O[r, 0, at, cols] + xb[r, 0, at, cols].astype(F32) + xb[r, 1, at, cols].astype(F32)
        return near + xd[r, at, cols].astype(F32) if r in (0, 2) else near

    def out_sum(r, rows=(0, ROWS), halves=(0, 1)):
        c.need(f"xb+{r}_0_0", f"xb-{r}_0_0")
        if r == 2:
            c.need(*(f"xd+2_{p}" for p in range(PARTS)))
        at, to = slice(*rows), pl.ds(rows[0], rows[1] - rows[0])
        cols = pl.ds(halves[0] * HALF, len(halves) * HALF)
        zs[r - 1, at, cols] = over_x(r, at, cols).astype(BF16)
        if r == 2:
            for p in range(PARTS):
                here, there = pl.ds(p * PART, PART), pl.ds(HALF + p * PART, PART)
                both = zt.at[:, :, here]
                c.send(f"z2+{p}", zs.at[1, :, here], zt.at[0, :, here], zp, both)
                c.send(f"z2-{p}", zs.at[1, :, there], zt.at[1, :, here], zm, both)
        else:
            name = f"z{r}_{rows[0]}_{halves[0]}"
            c.send(name, zs.at[r - 1, to, cols], zr.at[r - 1, to, cols], {1: zp, 3: zm}[r])

    def out_sum_far(p):
        here, there = pl.ds(p * PART, PART), pl.ds(HALF + p * PART, PART)
        both = zr.at[1, :, pl.ds(0, 2 * PART)]
        c.need(f"z2+{p}", f"z2-{p}")
        c.send(f"z2f+{p}", zt.at[0, :, here], zr.at[1, :, here], zp, both)
        c.send(f"z2f-{p}", zt.at[1, :, here], zr.at[1, :, there], zm, both)

    def out_final(first, rows):
        at = slice(first, first + rows)
        total = over_x(0, at, slice(0, WIDTH))
        for k in range(3):
            total += zr[k, at].astype(F32)
        out_ref[at] = total.astype(BF16)

    after = {
        1: ((out_near, 0, 1, (0, EARLY)), (out_near, 0, 3, (0, EARLY))),
        3: ((out_near, 1, 1), (out_near, 3, 3)),
        4: ((out_near, 1, 3), (out_near, 3, 1)),
        5: ((out_far, 2), (out_down, 1), (out_sum, 1, (0, EARLY)), (out_sum, 3, (0, EARLY))),
        6: ((out_down, 3), (out_near, 2, 1), (out_near, 2, 3)),
    }

    def run(events):
        for event, *args in events:
            event(*args)

    for n, (q, j) in enumerate(own):
        for k, (src, dst) in enumerate(pieces(q, j)):
            local(src, dst, weight_sems.at[2 * q + k // 2])
    for copy in own_tokens:
        copy.wait()
    forward(0, 0, 1)
    reduce_far(0)
    forward(0, 1, 4)
    reduce_near(0)
    relay_first("", ahead)
    forward(1)
    reduce_far(1)
    relay_first("b", behind)
    relay_1()
    grads(0)
    forward(2)
    reduce_far(2)
    reduce_near(1)
    spread(0)
    forward(3)
    reduce_far(3)
    reduce_near(2)
    relay_2()
    grads(1)
    backward(0)
    reduce_near(3)
    relay_3()
    forward(4)
    spread(1)
    grads(2)
    reduce_far(4)
    relay_4()
    grads(3)
    spread(2)
    backward(1)
    reduce_near(4)
    relays[5]()
    forward(5)
    spread(3)
    for t in range(5, last):
        reduce_far(t)
        if t == 5:
            backward(2)
        grads(t - 1)
        backward(t - 2, t)
        if t + 1 in relays:
            relays[t + 1]()
        forward(t + 1)
        spread(t - 1)
    reduce_far(last)
    grads(last - 1)
    for p in range(PARTS):
        out_pass(2, p)
    backward(last - 2, last)
    spread(last - 1)
    grads(last)
    backward(last - 1)
    spread(last)
    out_far(0)
    out_sum(2)

    def out_last(h):
        out_near(0, 1, (EARLY, ROWS), (h,))
        out_near(0, 3, (EARLY, ROWS), (h,))
        out_sum(1, (EARLY, ROWS), (h,))
        out_sum(3, (EARLY, ROWS), (h,))

    product(last, 0, 1)
    out_pass(0, 0)
    out_sum_far(0)
    product(last, 1, 1)
    out_last(0)
    out_pass(0, 1)
    out_sum_far(1)
    product(last, 2, 2)
    out_last(1)
    for copy in locals_:
        copy.wait_send()
    c.finish()
    out_final(0, ROWS // 2)
    out_final(ROWS // 2, ROWS // 2)


def shards(inputs, out_grad, gate_weight, up_weight, down_weight):
    return pl.pallas_call(
        kernel,
        out_shape=pltpu.VMEM((ROWS, WIDTH), BF16),
        in_specs=[pl.BlockSpec(memory_space=pl.ANY)] * 5,
        out_specs=pl.BlockSpec(memory_space=pltpu.VMEM),
        scratch_shapes=[
            pltpu.VMEM((4, 4, ROWS, WIDTH), BF16),
            pltpu.VMEM((4, 4, ROWS, WIDTH), BF16),
            pltpu.VMEM((WIDTH, 8 * Q), BF16),
            pltpu.VMEM((4 * Q, WIDTH), BF16),
            pltpu.VMEM((3, 4, TOP, 3 * Q), F32),
            pltpu.VMEM((4, 4, ROWS, WIDTH), F32),
            pltpu.VMEM((2, ALL, CUT), BF16),
            pltpu.VMEM((2, ALL, 3 * Q), BF16),
            pltpu.VMEM((ALL, 8 * Q), BF16),
            pltpu.VMEM((2, TOP, 3 * Q), BF16),
            pltpu.VMEM((2, 2, TOP, 3 * Q), BF16),
            pltpu.VMEM((4, ROWS, WIDTH), BF16),
            pltpu.VMEM((4, 2, ROWS, WIDTH), BF16),
            pltpu.VMEM((2, 2, ROWS, HALF), BF16),
            pltpu.VMEM((4, 2, ROWS, WIDTH), BF16),
            pltpu.VMEM((4, ROWS, WIDTH), BF16),
            pltpu.VMEM((3, ROWS, WIDTH), BF16),
            pltpu.VMEM((2, ROWS, HALF), BF16),
            pltpu.VMEM((3, ROWS, WIDTH), BF16),
            pltpu.SemaphoreType.DMA((SENDS,)),
            pltpu.SemaphoreType.DMA((RECVS,)),
            pltpu.SemaphoreType.DMA((2,)),
            pltpu.SemaphoreType.DMA((6,)),
            pltpu.SemaphoreType.DMA((8,)),
        ],
        compiler_params=pltpu.CompilerParams(
            collective_id=0, has_side_effects=True, vmem_limit_bytes=66_600_000
        ),
        name="swiglu_back",
    )(inputs, out_grad, gate_weight, up_weight, down_weight)


def solution(mesh):
    return jax.shard_map(
        shards,
        mesh=mesh,
        in_specs=(
            P(("gx", "gz"), "gy"),
            P(("gx", "gz"), "gy"),
            P("gy", ("gx", "gz")),
            P("gy", ("gx", "gz")),
            P(("gx", "gz"), "gy"),
        ),
        out_specs=P(("gx", "gz"), "gy"),
        check_vma=False,
    )
```
